32 devices in a mesh: wide: 8 (over z, x), narrow: 4 (over y, core).
Axes of the slice: x: 2, y: 2, z: 4, core: 2. Of those that a mesh axis runs over, the one named last changes fastest.
Arguments:
- rows: bfloat16 [8192, 1024], P(('wide', 'narrow')), may hold values from -6 to 6
- grades: int32 [8192], P(('wide', 'narrow')), may hold values from 0 to 4
- block_dest: int32 [32, 8], P(('wide', 'narrow')), may hold values from 0 to 7, each once within a row
- block_source: int32 [32, 8], P(('wide', 'narrow')), may hold values from 0 to 7, each once within a row
- lengths: int32 [8, 3], replicated, may hold values from 1 to 640, 1024 in all within a row
- gain: float32 [1024], replicated, may hold values from 0.5 to 1.5
- w_qkv: bfloat16 [1024, 3072], replicated, may hold values from -0.1875 to 0.1875
- w_out: bfloat16 [1024, 1024], replicated, may hold values from -0.1875 to 0.1875
- w_score: float32 [1024], replicated, may hold values from -0.1875 to 0.1875
Outputs:
- grad_rows: bfloat16 [8192, 1024], P(('wide', 'narrow'))
- grad_qkv: float32 [1024, 3072], P(None, ('wide', 'narrow'))
- grad_out: float32 [1024, 1024], P(None, ('wide', 'narrow'))
The draws below stay inside these ranges and needn't reach their ends.
Inputs may be any that keep to these rules, and one draw needn't show every extreme that they name: Each row of block_dest and of block_source names every group once. The lengths of one group sum to 1024.
All inputs are finite; a program needn't handle non-finite values.
Results may differ from the reference program's by a relative error of at most 0.0095.
Values may be sent and summed in bfloat16 or wider, within the bound.
No kernel may reach another device: no remote copies, remote signals or barrier semaphores. Data moves between devices by JAX's collectives and lax.ppermute only.
A program may use at most 128 MiB of HBM per device.

```python
import math
import jax
import jax.numpy as jnp
import numpy as np
from jax import lax

D = 1024
HEADS = 16
R_DEV = 256
LPG = 3
GROUP_ROWS = 1024
MOST_LEN = 640
NROWS = 8192
N_WIDE = 8
N_NARROW = 4


def touch_ends(entries, own_key, smallest, top_value):
    place = [jax.random.randint(jax.random.fold_in(own_key, axis), (), 0, length) for axis, length in enumerate(entries.shape)]
    widest = entries.shape.index(max(entries.shape))
    beside = place[:widest] + [(place[widest] + 1) % entries.shape[widest]] + place[widest + 1:]
    return entries.at[tuple(place)].set(smallest).at[tuple(beside)].set(top_value)


def block_levels(stream_key, shape, shards, low, high):
    level, own = 1.0, jax.random.fold_in(stream_key, 6)
    for position, parts in shards:
        steps = jnp.exp(jax.random.uniform(jax.random.fold_in(own, position), (parts,), jnp.float32, low / len(shards), high / len(shards)))
        level = level * jnp.repeat(steps, shape[position] // parts).reshape([-1 if axis == position else 1 for axis in range(len(shape))])
    return level


def profile(amount, total, bound, slope):
    loads = [(1 << 20) // math.isqrt(rank ** slope) + 1 for rank in range(2, amount + 1)]
    rest, holding = total - bound - (amount - 1), [1] * (amount - 1)
    while rest > 0:
        movable = [i for i in range(amount - 1) if holding[i] < bound]
        mass, remaining = sum([loads[i] for i in movable]), rest
        for i in movable:
            more = min(bound - holding[i], max(1, remaining * loads[i] // mass), rest)
            holding[i] = holding[i] + more
            rest = rest - more
    return np.array([bound] + holding)


def uneven_parts(stream_key, amount, total, reach, lean):
    if amount == 2:
        one = jax.random.randint(stream_key, (), max(1, total - reach), min(reach, total - 1) + 1)
        return jnp.stack([one, total - one])
    sizes = jnp.asarray(profile(amount, total, reach, lean), jnp.int32)
    pairs = (amount - 1) // 2
    giver, taker = sizes[1:1 + 2 * pairs:2], sizes[2:2 + 2 * pairs:2]
    slack = jnp.minimum(giver - 1, reach - taker)
    moved = jax.random.randint(jax.random.fold_in(stream_key, 1), (pairs,), 0, 1 << 20) % (slack + 1)
    sizes = sizes.at[1:1 + 2 * pairs:2].set(giver - moved).at[2:2 + 2 * pairs:2].set(taker + moved)
    return sizes[jax.random.permutation(jax.random.fold_in(stream_key, 2), amount)]


def centred(key, shape, deviation, limit, cuts=(), held_as=jnp.bfloat16):
    values = deviation * jax.random.normal(key, shape, jnp.float32)
    if cuts:
        values = values * block_levels(key, shape, cuts, -0.22, 0.18)
    return jnp.clip(values, -limit, limit).astype(held_as)


def setup_inputs(seed: int = 0) -> dict:
    key_of = jax.random.split(jax.random.key(seed), 10)
    return {
        "rows": centred(key_of[0], (NROWS, D), 1.0, 6.0, ((0, 32),)),
        "grades": touch_ends(jax.random.randint(key_of[1], (NROWS,), 0, 5), jax.random.fold_in(key_of[1], 1), 0, 4).astype(jnp.int32),
        "block_dest": jax.vmap(lambda own: jax.random.permutation(own, N_WIDE))(jax.random.split(key_of[2], (N_WIDE * N_NARROW))).reshape((N_WIDE * N_NARROW, N_WIDE)).astype(jnp.int32),
        "block_source": jax.vmap(lambda own: jax.random.permutation(own, N_WIDE))(jax.random.split(key_of[3], (N_WIDE * N_NARROW))).reshape((N_WIDE * N_NARROW, N_WIDE)).astype(jnp.int32),
        "lengths": jax.vmap(lambda own: uneven_parts(own, LPG, GROUP_ROWS, MOST_LEN, 2))(jax.random.split(key_of[4], N_WIDE)).reshape((N_WIDE, LPG)).astype(jnp.int32),
        "gain": jnp.clip(1.0 + 0.1 * jax.random.normal(key_of[5], (D,), jnp.float32), 0.5, 1.5),
        "w_qkv": centred(key_of[6], (D, 3 * D), D ** -0.5, 0.1875),
        "w_out": centred(key_of[7], (D, D), D ** -0.5, 0.1875),
        "w_score": centred(key_of[8], (D,), D ** -0.5, 0.1875, (), jnp.float32),
    }


epsilon = 1e-06
loss_scale = 64.0

def segment_ids(group_lengths, total):
    bounds = jnp.cumsum(group_lengths).astype(jnp.int32)
    positions = jnp.arange(total, dtype=jnp.int32)
    return lax.optimization_barrier(jnp.sum((positions[:, None] >= bounds[None, :]).astype(jnp.int32), axis=1))

def rounded(values):
    return lax.optimization_barrier(values.astype(jnp.bfloat16)).astype(jnp.float32)

def group_pass(work, grade_vals, segment, gain, w_qkv, w_out, w_score):
    total, width = work.shape
    head_size = width // HEADS
    scale = head_size ** (-0.5)
    rows_f32 = work.astype(jnp.float32)
    inverse = lax.rsqrt(lax.optimization_barrier(jnp.mean(rows_f32 * rows_f32, axis=1)) + epsilon)
    normed = (rows_f32 * inverse[:, None] * gain).astype(jnp.bfloat16)
    projected = jnp.dot(normed, w_qkv, preferred_element_type=jnp.float32).astype(jnp.bfloat16)
    proj_f32 = projected.astype(jnp.float32)
    queries = proj_f32[:, :width].reshape(total, HEADS, head_size)
    keys_all = proj_f32[:, width:2 * width].reshape(total, HEADS, head_size)
    values_all = proj_f32[:, 2 * width:].reshape(total, HEADS, head_size)
    same = (segment[:, None] == segment[None, :]).astype(jnp.float32)
    logits = jnp.einsum('qhd,khd->hqk', queries, keys_all) * scale
    weights = jnp.exp(logits) * same[None]
    totals = lax.optimization_barrier(jnp.sum(weights, axis=2))
    probs = weights / totals[:, :, None]
    probs_bf = rounded(probs)
    attended = jnp.einsum('hqk,khd->qhd', probs_bf, values_all).reshape(total, width).astype(jnp.bfloat16)
    hidden = rows_f32 + jnp.dot(attended, w_out, preferred_element_type=jnp.float32)
    scores = jnp.dot(hidden, w_score, precision=lax.Precision.HIGHEST)
    gains = jnp.exp2(grade_vals.astype(jnp.float32))
    norm_sum = jnp.dot(same, gains, precision=lax.Precision.HIGHEST)
    spread = gains[:, None] - gains[None, :]
    margins = scores[:, None] - scores[None, :]
    upper = jnp.maximum(spread, 0.0) * same
    lower = jnp.maximum(-spread, 0.0) * same
    score_grad = loss_scale * lax.optimization_barrier(jnp.sum(lower * jax.nn.sigmoid(margins) - upper * jax.nn.sigmoid(-margins), axis=1)) / norm_sum
    hidden_grad = score_grad[:, None] * w_score[None, :]
    hidden_bf = hidden_grad.astype(jnp.bfloat16)
    out_grad = jnp.dot(attended.T, hidden_bf, preferred_element_type=jnp.float32)
    upstream = jnp.dot(hidden_bf, w_out.T, preferred_element_type=jnp.float32).astype(jnp.bfloat16)
    upstream_f32 = upstream.astype(jnp.float32).reshape(total, HEADS, head_size)
    attended_f32 = attended.astype(jnp.float32).reshape(total, HEADS, head_size)
    delta = lax.optimization_barrier(jnp.sum(upstream_f32 * attended_f32, axis=2))
    prob_grad = jnp.einsum('qhd,khd->hqk', upstream_f32, values_all)
    logit_grad = rounded(probs * (prob_grad - delta.T[:, :, None]) * scale)
    query_grad = jnp.einsum('hqk,khd->qhd', logit_grad, keys_all).reshape(total, width)
    key_grad = jnp.einsum('hqk,qhd->khd', logit_grad, queries).reshape(total, width)
    value_grad = jnp.einsum('hqk,qhd->khd', probs_bf, upstream_f32).reshape(total, width)
    proj_grad = jnp.concatenate([query_grad, key_grad, value_grad], axis=1).astype(jnp.bfloat16)
    qkv_grad = jnp.dot(normed.T, proj_grad, preferred_element_type=jnp.float32)
    normed_grad = jnp.dot(proj_grad, w_qkv.T, preferred_element_type=jnp.float32)
    scaled = normed_grad * gain
    row_grad = hidden_grad + inverse[:, None] * scaled - rows_f32 * (inverse ** 3)[:, None] * lax.optimization_barrier(jnp.mean(scaled * rows_f32, axis=1))[:, None]
    return (row_grad.astype(jnp.bfloat16), qkv_grad, out_grad)

def reference(rows, grades, block_dest, block_source, lengths, gain, w_qkv, w_out, w_score):
    width = rows.shape[1]
    piece = R_DEV // N_WIDE
    group_total = R_DEV * N_NARROW
    blocks = rows.reshape(N_WIDE * N_NARROW * N_WIDE, piece, width)
    grade_blocks = grades.reshape(N_WIDE * N_NARROW * N_WIDE, piece)
    dest = block_dest.reshape(N_WIDE, N_NARROW, N_WIDE)
    source = block_source.reshape(N_WIDE, N_NARROW, N_WIDE)
    slots = jnp.arange(N_WIDE, dtype=jnp.int32)
    dest_inverse = lax.optimization_barrier(jnp.sum(slots[None, None, None, :] * (dest[:, :, None, :] == slots[None, None, :, None]).astype(jnp.int32), axis=3))
    narrow_ids = jnp.arange(N_NARROW, dtype=jnp.int32)[None, :, None]
    group_ids = slots[:, None, None]
    chosen = dest_inverse[source, narrow_ids, group_ids]
    index = ((source * N_NARROW + narrow_ids) * N_WIDE + chosen).reshape(-1).astype(jnp.int32)
    work_rows = blocks[index].reshape(N_WIDE, group_total, width)
    work_grades = grade_blocks[index].reshape(N_WIDE, group_total)

    def step(carry, inputs):
        group_rows, group_grades, group_lengths = inputs
        segment = segment_ids(group_lengths, group_total)
        row_grad, qkv_grad, out_grad = group_pass(group_rows, group_grades, segment, gain, w_qkv, w_out, w_score)
        return ((carry[0] + qkv_grad, carry[1] + out_grad), row_grad)
    start = (jnp.zeros((width, 3 * width), jnp.float32), jnp.zeros((width, width), jnp.float32))
    (qkv_total, out_total), work_grads = lax.scan(step, start, (work_rows, work_grades, lengths))
    home = jnp.zeros_like(blocks).at[index].set(work_grads.reshape(-1, piece, width))
    return (home.reshape(rows.shape), qkv_total, out_total)
```

```python
import jax
import jax.numpy as jnp
from jax import lax
from jax.experimental import pallas as pl
from jax.experimental.pallas import tpu as pltpu
from jax.sharding import PartitionSpec as P

HEADS = 16
LANES = 128
epsilon = 1e-06
loss_scale = 64.0
log2e = 1.4426950408889634
far = 2.0**100
bf16 = jnp.bfloat16
f32 = jnp.float32


def vmem():
    return pl.BlockSpec(memory_space=pltpu.VMEM)


def smem():
    return pl.BlockSpec(memory_space=pltpu.SMEM)


def call(kernel, shapes, specs, **more):
    params = pltpu.CompilerParams(vmem_limit_bytes=56 * 2**20)
    return pl.pallas_call(kernel, out_shape=shapes, in_specs=specs, compiler_params=params, **more)


def split(values):
    high = values.astype(bf16)
    return high, (values - high.astype(f32)).astype(bf16)


def pack_kernel(dest, rows, grades, out):
    count, piece, width = rows.shape
    for b in range(count):
        out[dest[0, b], :, :width] = rows[b]
        out[dest[0, b], :, width:] = jnp.broadcast_to(grades[b], (piece, LANES)).astype(bf16)


def norm_kernel(source, incoming, gain, score, out, inverse_out, rows_out):
    count, piece, wide = incoming.shape
    width = wide - LANES
    lane = lax.broadcasted_iota(jnp.int32, (piece, LANES), 1)
    for c in range(count):
        block = incoming[source[0, c]]
        rows = block[:, :width]
        values = rows.astype(f32)
        inverse = lax.rsqrt(jnp.mean(values * values, axis=1, keepdims=True) + epsilon)
        out[c, :, :width] = (values * inverse * gain[...]).astype(bf16)
        base = jnp.sum(values * score[...], axis=1, keepdims=True)
        high = base.astype(bf16).astype(f32)
        middle = (base - high).astype(bf16).astype(f32)
        low = base - high - middle
        info = jnp.where(lane == 1, high, block[:, width:].astype(f32))
        info = jnp.where(lane == 2, middle, info)
        info = jnp.where(lane == 3, low, info)
        out[c, :, width:] = info.astype(bf16)
        inverse_out[c] = inverse
        rows_out[c] = rows


def project_kernel(x, weights, qk_out, z_out):
    both = qk_out.shape[1]
    out = jnp.dot(x[:, : x.shape[1] - LANES], weights[...], preferred_element_type=f32)
    qk_out[...] = out[:, :both].astype(bf16)
    z_out[...] = out[:, both:]


def forward_kernel(query, key, z, seg_col, seg_all, a_out, e_out, stat_out, zrow_out, kx, zt):
    total = key.shape[0]
    rows = query.shape[0]
    heads = e_out.shape[0]
    half = LANES // 2

    @pl.when(pl.program_id(0) == 0)
    def _():
        lane = lax.broadcasted_iota(jnp.int32, (total, LANES), 1)
        away = jnp.where(lane == seg_all[...], 0.0, -far).astype(bf16)
        for p in range(heads // 2):
            kx[p, :, :LANES] = key[:, p * LANES : (p + 1) * LANES]
            kx[p, :, LANES:] = away
        turned = z[...].T
        zt[...] = turned[:8] + turned[8:16]
        zrow_out[...] = zt[...]

    lane = lax.broadcasted_iota(jnp.int32, (rows, LANES), 1)
    mine = (lane == seg_col[...]).astype(f32).astype(bf16)
    stats = jnp.zeros((rows, LANES), f32)
    zsum = jnp.zeros((rows, 1), f32)
    for p in range(heads // 2):
        parts = []
        for s in range(2):
            h = 2 * p + s
            own = query[:, p * LANES : (p + 1) * LANES]
            own = jnp.where((lane >= half) == (s == 1), own, jnp.zeros_like(own))
            logits = lax.dot_general(
                jnp.concatenate([own, mine], axis=1),
                kx[p],
                (((1,), (1,)), ((), ())),
                preferred_element_type=f32,
            )
            weights = jnp.exp2(logits * log2e)
            e_out[h] = weights.astype(bf16)
            zrow = zt[h : h + 1, :]
            inverse = 1.0 / jnp.sum(weights, axis=1, keepdims=True)
            zeta = jnp.sum(weights * zrow, axis=1, keepdims=True) * inverse
            centred = (weights * (zrow - zeta)).astype(bf16)
            part = jnp.dot(centred, kx[p, :, :LANES], preferred_element_type=f32) * inverse
            parts.append(part)
            stats = jnp.where(lane == h, zeta, stats)
            stats = jnp.where(lane == heads + h, inverse, stats)
            zsum = zsum + zeta
        a_out[:, p * LANES : (p + 1) * LANES] = jnp.where(lane >= half, parts[1], parts[0])
    stat_out[...] = jnp.where(lane == 2 * heads, zsum, stats)


def backward_kernel(
    e, stat, query, a, zrow, s_col, s_row, g_col, g_row, t_col, t_row,
    key_out, c_out, qg_out, sg_out, key_acc, c_acc,
):
    heads, rows, total = e.shape
    half = LANES // 2
    scale = half**-0.5
    step = pl.program_id(0)

    @pl.when(step == 0)
    def _():
        key_acc[...] = jnp.zeros_like(key_acc)
        c_acc[...] = jnp.zeros_like(c_acc)

    lane = lax.broadcasted_iota(jnp.int32, (rows, LANES), 1)
    same = t_col[...] == t_row[...]
    gains = g_row[...]
    spread = gains - g_col[...]
    margin = s_col[...] - s_row[...]
    margin = jnp.where(spread > 0.0, margin, -margin)
    pulls = spread / (1.0 + jnp.exp(-margin))
    pulls = jnp.sum(jnp.where(same, pulls, 0.0), axis=1, keepdims=True)
    norm = jnp.sum(jnp.where(same, gains, 0.0), axis=1, keepdims=True)
    grad = loss_scale * pulls / norm
    sg_out[...] = grad
    qg_out[...] = (a[...] * (grad * scale)).astype(bf16)
    stats = stat[...]
    for h in range(heads):
        p, s = h // 2, h % 2
        zeta = stats[:, h : h + 1]
        scaled = e[h].astype(f32) * (stats[:, heads + h : heads + h + 1] * grad)
        c_acc[h : h + 1, :] += jnp.sum(scaled, axis=0, keepdims=True)
        centred = (scaled * (zrow[h : h + 1, :] - zeta)).astype(bf16)
        own = query[:, p * LANES : (p + 1) * LANES]
        own = jnp.where((lane >= half) == (s == 1), own, jnp.zeros_like(own))
        key_acc[p * LANES : (p + 1) * LANES, :] += lax.dot_general(
            own, centred, (((0,), (0,)), ((), ())), preferred_element_type=f32
        )

    @pl.when(step == pl.num_programs(0) - 1)
    def _():
        key_out[...] = key_acc[...].astype(bf16)
        c_out[...] = c_acc[...]


def tail_kernel(source, normed_grad, rows, inverse, grad, gain, score, out):
    count, piece, width = out.shape
    for c in range(count):
        part = pl.ds(c * piece, piece)
        scaled = normed_grad[part, :] * gain[...]
        values = rows[c].astype(f32)
        inv = inverse[c]
        mean = jnp.mean(scaled * values, axis=1, keepdims=True)
        total = grad[part, :] * score[...] + inv * scaled - values * (inv * inv * inv * mean)
        out[source[0, c]] = total.astype(bf16)


def body(rows, grades, block_dest, block_source, lengths, gain, w_qkv, w_out, w_score):
    wide = lax.axis_size("wide")
    narrow = lax.axis_size("narrow")
    wide_index = lax.axis_index("wide")
    narrow_index = lax.axis_index("narrow")
    local, width = rows.shape
    piece = local // wide
    head_size = width // HEADS
    heads = HEADS // narrow
    own = heads * head_size
    total = local * narrow
    chunk = width // wide
    scale = head_size**-0.5
    order = jnp.bitwise_xor(narrow_index, jnp.arange(narrow, dtype=jnp.int32))

    def swap(values, m):
        return lax.ppermute(values, "narrow", [(i, i ^ m) for i in range(narrow)])

    def spread(values):
        held = [values]
        step = 1
        while step < narrow:
            held = held + [None] * len(held)
            held[step] = swap(values, step)
            step *= 2
        for m in range(narrow):
            if held[m] is None:
                top = 1 << (m.bit_length() - 1)
                held[m] = swap(held[top], m ^ top)
        return held

    u = jnp.sum(w_out.astype(f32) * w_score[None, :], axis=1)
    w_q = w_qkv[:, :width].reshape(width, narrow, own)[:, order].reshape(width, width)
    w_k = w_qkv[:, width : 2 * width].reshape(width, narrow, own)[:, order].reshape(width, width)
    head_of = jnp.arange(width, dtype=jnp.int32) // head_size
    head_order = (order[:, None] * heads + jnp.arange(heads, dtype=jnp.int32)[None, :]).reshape(-1)
    u_heads = jnp.where(head_of[:, None] == head_order[None, :], u[:, None], 0.0)
    u_high, u_low = split(u_heads)
    g_both = jnp.dot(
        w_qkv[:, 2 * width :], jnp.concatenate([u_high, u_low], axis=1), preferred_element_type=f32
    )
    g_all = g_both[:, :HEADS] + g_both[:, HEADS:]
    g_high, g_low = split(g_all[:, :heads])
    pad = jnp.zeros((width, 8 - heads), bf16)
    g_own = jnp.concatenate([g_high, pad, g_low, pad, jnp.zeros((width, LANES - 16), bf16)], axis=1)
    weights = jnp.concatenate([w_q[:, :own] * bf16(scale), w_k[:, :own], g_own], axis=1)

    outgoing = call(
        pack_kernel,
        jax.ShapeDtypeStruct((wide, piece, width + LANES), bf16),
        [smem(), vmem(), vmem()],
    )(
        block_dest,
        rows.reshape(wide, piece, width),
        grades.astype(f32).reshape(wide, piece, 1),
    )
    incoming = lax.all_to_all(outgoing, "wide", split_axis=0, concat_axis=0, tiled=True)
    normx, inverse, work = call(
        norm_kernel,
        (
            jax.ShapeDtypeStruct((wide, piece, width + LANES), bf16),
            jax.ShapeDtypeStruct((wide, piece, 1), f32),
            jax.ShapeDtypeStruct((wide, piece, width), bf16),
        ),
        [smem(), vmem(), vmem(), vmem()],
    )(block_source, incoming, gain[None, :], w_score[None, :])
    x_all = jnp.concatenate(spread(normx.reshape(local, width + LANES)), axis=0)
    qk, z = call(
        project_kernel,
        (
            jax.ShapeDtypeStruct((total, 2 * own), bf16),
            jax.ShapeDtypeStruct((total, LANES), f32),
        ),
        [
            pl.BlockSpec((local, width + LANES), lambda i: (i, 0)),
            pl.BlockSpec((width, 2 * own + LANES), lambda i: (0, 0)),
        ],
        grid=(narrow,),
        out_specs=(
            pl.BlockSpec((local, 2 * own), lambda i: (i, 0)),
            pl.BlockSpec((local, LANES), lambda i: (i, 0)),
        ),
    )(x_all, weights)

    bounds = jnp.cumsum(lax.dynamic_index_in_dim(lengths, wide_index, 0, keepdims=False))
    positions = (order[:, None] * local + jnp.arange(local, dtype=jnp.int32)[None, :]).reshape(-1)
    segment = jnp.sum((positions[:, None] >= bounds[None, :]).astype(jnp.int32), axis=1)

    column = pl.BlockSpec((local, 1), lambda i: (i, 0))
    line = pl.BlockSpec((1, total), lambda i: (0, 0))
    a, e, stat, zrow = call(
        forward_kernel,
        (
            jax.ShapeDtypeStruct((total, own), f32),
            jax.ShapeDtypeStruct((heads, total, total), bf16),
            jax.ShapeDtypeStruct((total, LANES), f32),
            jax.ShapeDtypeStruct((8, total), f32),
        ),
        [
            pl.BlockSpec((local, own), lambda i: (i, 0)),
            pl.BlockSpec((total, own), lambda i: (0, 1)),
            pl.BlockSpec((total, LANES), lambda i: (0, 0)),
            column,
            pl.BlockSpec((total, 1), lambda i: (0, 0)),
        ],
        grid=(narrow,),
        out_specs=(
            pl.BlockSpec((local, own), lambda i: (i, 0)),
            pl.BlockSpec((heads, local, total), lambda i: (0, i, 0)),
            pl.BlockSpec((local, LANES), lambda i: (i, 0)),
            pl.BlockSpec((8, total), lambda i: (0, 0)),
        ),
        scratch_shapes=[
            pltpu.VMEM((heads // 2, total, 2 * LANES), bf16),
            pltpu.VMEM((8, total), f32),
        ],
    )(qk, qk, z, segment[:, None], segment[:, None])

    info = x_all[:, width : width + 4].astype(f32)
    partial = stat[:, 2 * heads].reshape(narrow, local)
    step = 1
    while step < narrow:
        other = swap(partial, step)
        partial = partial + jnp.stack([other[m ^ step] for m in range(narrow)])
        step *= 2
    scores = info[:, 1] + info[:, 2] + info[:, 3] + partial.reshape(total)
    gains = jnp.exp2(info[:, 0])

    a_bf = a.astype(bf16)
    a_rows = [a_bf[:local]] + [swap(a_bf[m * local : (m + 1) * local], m) for m in range(1, narrow)]
    a_rows = jnp.concatenate(a_rows, axis=1)

    key_t, c_t, query_grad, score_grad = call(
        backward_kernel,
        (
            jax.ShapeDtypeStruct((own, total), bf16),
            jax.ShapeDtypeStruct((8, total), f32),
            jax.ShapeDtypeStruct((total, own), bf16),
            jax.ShapeDtypeStruct((total, 1), f32),
        ),
        [
            pl.BlockSpec((heads, local, total), lambda i: (0, i, 0)),
            pl.BlockSpec((local, LANES), lambda i: (i, 0)),
            pl.BlockSpec((local, own), lambda i: (i, 0)),
            pl.BlockSpec((local, own), lambda i: (i, 0)),
            pl.BlockSpec((8, total), lambda i: (0, 0)),
            column,
            line,
            column,
            line,
            column,
            line,
        ],
        grid=(narrow,),
        out_specs=(
            pl.BlockSpec((own, total), lambda i: (0, 0)),
            pl.BlockSpec((8, total), lambda i: (0, 0)),
            pl.BlockSpec((local, own), lambda i: (i, 0)),
            column,
        ),
        scratch_shapes=[pltpu.VMEM((own, total), f32), pltpu.VMEM((8, total), f32)],
    )(
        e, stat, qk, a, zrow,
        scores[:, None], scores[None, :],
        gains[:, None], gains[None, :],
        segment[:, None], segment[None, :],
    )

    c_high, c_low = split(c_t[:heads])
    keys_c = jnp.concatenate([key_t, c_high, c_low, jnp.zeros((8, total), bf16)], axis=0)
    k_rows = [keys_c[:, :local]]
    k_rows += [swap(keys_c[:, m * local : (m + 1) * local], m) for m in range(1, narrow)]
    c_rows = jnp.concatenate(
        [r[own : own + heads].astype(f32) + r[own + heads : own + 2 * heads].astype(f32) for r in k_rows]
    )
    k_rows = jnp.concatenate([r[:own] for r in k_rows], axis=0)

    normed_all = x_all[:, :width]
    grad_q = lax.dot_general(
        query_grad, normed_all, (((0,), (0,)), ((), ())), preferred_element_type=f32
    )
    grad_k = jnp.dot(keys_c, normed_all, preferred_element_type=f32)
    m_own = grad_k[own : own + heads] + grad_k[own + heads : own + 2 * heads]
    w_v = lax.dynamic_slice_in_dim(w_qkv, 2 * width + narrow_index * own, own, axis=1)
    m_high, m_low = split(m_own)
    v_both = jnp.dot(jnp.concatenate([m_high, m_low]), w_v, preferred_element_type=f32)
    v_heads = v_both[:heads] + v_both[heads:]
    own_head = jnp.arange(own, dtype=jnp.int32) // head_size
    v_own = jnp.sum(
        jnp.where(own_head[None, :] == jnp.arange(heads, dtype=jnp.int32)[:, None], v_heads, 0.0), axis=0
    )

    def to_chunks(values):
        return values.reshape(-1, wide, chunk).transpose(1, 0, 2)

    v_high, v_low = split(v_own)
    v_lines = jnp.concatenate([v_high, v_low]).reshape(1, -1, chunk)
    count_v = v_lines.shape[1]
    blocks = [
        to_chunks(jnp.concatenate([grad_q, grad_k[:own]]).astype(bf16)),
        to_chunks(jnp.concatenate([m_high, m_low])),
        jnp.broadcast_to(v_lines, (wide, count_v, chunk)),
    ]
    fill = -(2 * own + 2 * heads + count_v) % 16
    blocks.append(jnp.zeros((wide, fill, chunk), bf16))
    terms = lax.all_to_all(
        jnp.concatenate(blocks, axis=1), "wide", split_axis=0, concat_axis=0, tiled=True
    )
    summed = jnp.sum(terms.astype(f32), axis=0)

    def both(values):
        n = values.shape[0] // 2
        return values[:n] + values[n:]

    at = 2 * own + 2 * heads
    m_high, m_low = split(both(summed[2 * own : at]))
    v_sum = both(summed[at : at + count_v])
    v_high, v_low = split(v_sum)
    send = jnp.concatenate([summed[: 2 * own].astype(bf16), m_high, m_low, v_high, v_low], axis=0)
    gathered = jnp.stack(spread(send))[order]
    q_cols = gathered[:, :own].reshape(width, chunk)
    k_cols = gathered[:, own : 2 * own].reshape(width, chunk)
    m_all = gathered[:, 2 * own : 2 * own + heads].astype(f32) + gathered[:, 2 * own + heads : at].astype(f32)
    m_rows = jnp.broadcast_to(m_all.reshape(HEADS, 1, chunk), (HEADS, head_size, chunk))
    v_cols = (m_rows.reshape(width, chunk) * u[:, None]).astype(bf16)
    half_v = count_v // 2
    v_all = gathered[:, at : at + half_v].astype(f32) + gathered[:, at + half_v : at + count_v].astype(f32)
    v_all = v_all.reshape(width)
    columns = 3 * width // (wide * narrow)
    full = jnp.concatenate([q_cols, k_cols, v_cols], axis=0).reshape(wide, narrow, columns, chunk)
    mine = lax.dynamic_index_in_dim(full, narrow_index, 1, keepdims=False)
    parts = lax.all_to_all(mine, "wide", split_axis=0, concat_axis=0, tiled=True)
    grad_qkv = parts.astype(f32).transpose(0, 2, 1).reshape(width, columns)
    out_columns = width // (wide * narrow)
    place = (wide_index * narrow + narrow_index) * out_columns
    grad_out = v_all[:, None] * lax.dynamic_slice_in_dim(w_score, place, out_columns)[None, :]

    own_grad = score_grad[:local]
    normed_grad = own_grad * scale * jnp.einsum("rd,ed->re", a_rows, w_q, preferred_element_type=f32)
    normed_grad = normed_grad + jnp.einsum("dr,ed->re", k_rows, w_k, preferred_element_type=f32)
    normed_grad = normed_grad + jnp.einsum(
        "hr,eh->re", c_rows, g_all, precision=lax.Precision.HIGHEST, preferred_element_type=f32
    )
    returning = call(
        tail_kernel,
        jax.ShapeDtypeStruct((wide, piece, width), bf16),
        [smem()] + [vmem()] * 6,
    )(block_source, normed_grad, work, inverse, own_grad, gain[None, :], w_score[None, :])
    arrived = lax.all_to_all(returning, "wide", split_axis=0, concat_axis=0, tiled=True)
    grad_rows = arrived[block_dest[0]].reshape(local, width)
    return (grad_rows, grad_qkv, grad_out)


def solution(mesh):
    both = ("wide", "narrow")
    placed = (P(both, None), P(both), P(both, None), P(both, None), P(), P(), P(), P(), P())
    return jax.shard_map(
        body,
        mesh=mesh,
        in_specs=placed,
        out_specs=(P(both, None), P(None, both), P(None, both)),
        check_vma=False,
    )
```

```python
import jax
import jax.numpy as jnp
from jax import lax
from jax.experimental import pallas as pl
from jax.experimental.pallas import tpu as pltpu
from jax.sharding import PartitionSpec as P


HEADS = 16
LANES = 128
epsilon = 1e-06
loss_scale = 64.0
log2e = 1.4426950408889634
far = 2.0**100
bf16 = jnp.bfloat16
f32 = jnp.float32


def vmem():
    return pl.BlockSpec(memory_space=pltpu.VMEM)


def smem():
    return pl.BlockSpec(memory_space=pltpu.SMEM)


def whole(shape):
    return pl.BlockSpec(shape, lambda *_: (0,) * len(shape))


def call(kernel, shapes, specs, work=0, room=8, **more):
    params = pltpu.CompilerParams(vmem_limit_bytes=room * 2**20)
    cost = pl.CostEstimate(flops=work, transcendentals=0, bytes_accessed=0)
    return pl.pallas_call(
        kernel, out_shape=shapes, in_specs=specs, compiler_params=params, cost_estimate=cost, **more
    )


def indexed(kernel, shapes, specs, out_specs, grid, scratch=(), work=0, room=8):
    params = pltpu.CompilerParams(vmem_limit_bytes=room * 2**20)
    cost = pl.CostEstimate(flops=work, transcendentals=0, bytes_accessed=0)
    spec = pltpu.PrefetchScalarGridSpec(
        num_scalar_prefetch=1, grid=grid, in_specs=specs, out_specs=out_specs, scratch_shapes=scratch
    )
    return pl.pallas_call(
        kernel, out_shape=shapes, grid_spec=spec, compiler_params=params, cost_estimate=cost
    )


def near(values):
    return pltpu.with_memory_space_constraint(values, pltpu.VMEM)


def stay(values):
    return pltpu.with_memory_space_constraint(values, pltpu.HBM)


def contract(left, right, dims, **more):
    return lax.dot_general(left, right, (dims, ((), ())), preferred_element_type=f32, **more)


def prepare_kernel(w_v, w_out, score, u_out, turned_out, proj_out):
    width = w_v.shape[0]
    half = LANES // 2
    u = jnp.sum(w_out[...].astype(f32) * score[...], axis=1, keepdims=True)
    u_out[...] = u
    high = u.astype(bf16).astype(f32)
    lane = lax.broadcasted_iota(jnp.int32, (width, LANES), 1)
    head = lax.broadcasted_iota(jnp.int32, (width, LANES), 0) // (width // HEADS)
    columns = jnp.where(lane == head, high, 0.0)
    columns = jnp.where(lane == half + head, u - high, columns).astype(bf16)
    g = jnp.dot(w_v[...], columns, preferred_element_type=f32)
    g = g + pltpu.roll(g, half, axis=1)
    high = g.astype(bf16).astype(f32)
    tops, rests = high.T[:HEADS], (g - high).T[:HEADS]
    turned_out[...] = jnp.concatenate([tops, tops, rests], axis=0).astype(bf16)
    proj_out[...] = jnp.where(lane < half, high, g - high).astype(bf16)


def pack_kernel(dest, rows, grades, out):
    count, piece, width = rows.shape
    total = grades.shape[1]
    row = lax.broadcasted_iota(jnp.int32, (piece, total), 0)
    lane = lax.broadcasted_iota(jnp.int32, (piece, total), 1)
    line = grades[...].astype(f32)
    for b in range(count):
        grade = jnp.sum(jnp.where(lane == row + b * piece, line, 0.0), axis=1, keepdims=True)
        out[dest[0, b], :, :width] = rows[b]
        out[dest[0, b], :, width:] = jnp.broadcast_to(grade, (piece, LANES)).astype(bf16)


def norm_kernel(source, table, incoming, gain, score, ready, out):
    count, piece, wide = incoming.shape
    width = wide - LANES
    lane = lax.broadcasted_iota(jnp.int32, (piece, LANES), 1)
    for c in range(count):
        block = incoming[source[0, c]]
        values = block[:, :width].astype(f32)
        inverse = lax.rsqrt(jnp.mean(values * values, axis=1, keepdims=True) + epsilon)
        out[c, :, :width] = (values * inverse * gain[...]).astype(bf16)
        base = jnp.sum(values * score[...], axis=1, keepdims=True)
        high = base.astype(bf16).astype(f32)
        middle = (base - high).astype(bf16).astype(f32)
        low = base - high - middle
        info = jnp.where(lane == 1, high, block[:, width:].astype(f32))
        info = jnp.where(lane == 2, middle, info)
        info = jnp.where(lane == 3, low, info)
        out[c, :, width:] = info.astype(bf16)


def list_of(table, narrow, lists, first, shape, axis):
    position = lax.broadcasted_iota(jnp.int32, shape, axis) + first
    found = jnp.zeros(shape, jnp.int32)
    for s in range(lists):
        found = found + (position >= table[narrow + s]).astype(jnp.int32)
    return found


def forward_kernel(table, *refs, narrow, lists):
    blocks = refs[:narrow]
    w_q, w_k, g, k_out, e_out, q_out, x_out, stat_out, part_out, z_out, lines_out, xs, qs, kx, zt = refs[narrow:]
    local = blocks[0].shape[0]
    width = w_q.shape[0]
    heads = e_out.shape[0]
    half = LANES // 2
    scale = half**-0.5
    step = pl.program_id(0)

    @pl.when(step == 0)
    def _():
        lane = lax.broadcasted_iota(jnp.int32, (local, LANES), 1)
        for m in range(narrow):
            rows = pl.ds(m * local, local)
            block = blocks[m][:, :width]
            xs[rows, :] = blocks[m][...]
            qs[rows, :] = (jnp.dot(block, w_q[...], preferred_element_type=f32) * scale).astype(bf16)
            keys = jnp.dot(block, w_k[...], preferred_element_type=f32).astype(bf16)
            segment = list_of(table, narrow, lists, table[m] * local, (local, LANES), 0)
            away = jnp.where(lane == segment, 0.0, -far).astype(bf16)
            for p in range(heads // 2):
                kx[p, rows, :LANES] = keys[:, p * LANES : (p + 1) * LANES]
                kx[p, rows, LANES:] = away
            k_out[rows, :] = keys
            turned = jnp.dot(block, g[...], preferred_element_type=f32).T
            zt[:, rows] = turned[:HEADS] + turned[half : half + HEADS]
            info = blocks[m][:, width:].astype(f32).T
            lines_out[0:1, rows] = info[1:2] + info[2:3] + info[3:4]
            lines_out[1:2, rows] = jnp.exp2(info[0:1])
            lines_out[2:3, rows] = list_of(table, narrow, lists, table[m] * local, (1, local), 1).astype(f32)
        z_out[...] = zt[...]

    at = pl.ds(pl.multiple_of(step * local, local), local)
    query = qs[at, :]
    q_out[...] = query
    x_out[...] = xs[at, :]
    lane = lax.broadcasted_iota(jnp.int32, (local, LANES), 1)
    segment = list_of(table, narrow, lists, table[step] * local, (local, LANES), 0)
    mine = (lane == segment).astype(f32).astype(bf16)
    stats = jnp.zeros((local, LANES), f32)
    zsum = jnp.zeros((local, 1), f32)
    for p in range(heads // 2):
        for s in range(2):
            h = 2 * p + s
            own = query[:, p * LANES : (p + 1) * LANES]
            own = jnp.where((lane >= half) == (s == 1), own, jnp.zeros_like(own))
            logits = contract(jnp.concatenate([own, mine], axis=1), kx[p], ((1,), (1,)))
            weights = jnp.exp2(logits * log2e)
            e_out[h] = weights.astype(bf16)
            zrow = zt[pl.ds(table[0] * heads + h, 1), :]
            inverse = 1.0 / jnp.sum(weights, axis=1, keepdims=True)
            zeta = jnp.sum(weights * zrow, axis=1, keepdims=True) * inverse
            stats = jnp.where(lane == h, zeta, stats)
            stats = jnp.where(lane == heads + h, inverse, stats)
            zsum = zsum + zeta
    stat_out[...] = stats
    part_out[...] = jnp.broadcast_to(zsum, (local, LANES)).T[:1]


def center_kernel(table, e, stat, key, z, a_out):
    heads = e.shape[0]
    rows = stat.shape[0]
    half = LANES // 2
    here = pl.ds(pl.multiple_of(pl.program_id(0) * rows, rows), rows)
    lane = lax.broadcasted_iota(jnp.int32, (rows, LANES), 1)
    stats = stat[...]
    for p in range(heads // 2):
        at = slice(p * LANES, (p + 1) * LANES)
        parts = []
        for h in (2 * p, 2 * p + 1):
            zrow = z[pl.ds(table[0] * heads + h, 1), :]
            centred = (e[h, here, :].astype(f32) * (zrow - stats[:, h : h + 1])).astype(bf16)
            part = jnp.dot(centred, key[:, at], preferred_element_type=f32)
            parts.append(part * stats[:, heads + h : heads + h + 1])
        a_out[:, at] = jnp.where(lane >= half, parts[1], parts[0]).astype(bf16)


def score_kernel(table, *refs, narrow):
    partials = refs[:narrow]
    given, x, a, grad_out, gq_out, lines, acc = refs[narrow:]
    local, _ = a.shape
    width = x.shape[1] - LANES
    scale = (LANES // 2) ** -0.5
    wide, _, chunk = gq_out.shape
    step = pl.program_id(0)

    @pl.when(step == 0)
    def _():
        acc[...] = jnp.zeros_like(acc)
        lines[...] = given[...]
        for m in range(narrow):
            rows = pl.ds(m * local, local)
            summed = given[0:1, rows]
            for d in range(narrow):
                summed = summed + partials[d][:, (m ^ d) * local : ((m ^ d) + 1) * local]
            lines[0:1, rows] = summed

    at = pl.ds(pl.multiple_of(step * local, local), local)
    turned = jnp.concatenate([lines[:, at]] * (LANES // 8), axis=0).T
    same = turned[:, 2:3] == lines[2:3, :]
    gains = lines[1:2, :]
    spread = gains - turned[:, 1:2]
    margin = turned[:, 0:1] - lines[0:1, :]
    margin = jnp.where(spread > 0.0, margin, -margin)
    pulls = spread / (1.0 + jnp.exp(-margin))
    pulls = jnp.sum(jnp.where(same, pulls, 0.0), axis=1, keepdims=True)
    norm = jnp.sum(jnp.where(same, gains, 0.0), axis=1, keepdims=True)
    grad = loss_scale * pulls / norm
    grad_out[...] = grad
    query = (a[...].astype(f32) * (grad * scale)).astype(bf16)
    acc[...] += contract(query, x[:, :width], ((0,), (0,)))

    @pl.when(step == pl.num_programs(0) - 1)
    def _():
        for w in range(wide):
            gq_out[w] = acc[:, w * chunk : (w + 1) * chunk].astype(bf16)


def key_kernel(table, e, stat, query, z, grad, w_v, x_hbm, keys_out, keep_out, send_out, x, key_acc, c_acc, sem, at_wide):
    heads, total, _ = e.shape
    rows = query.shape[0]
    half = LANES // 2
    own = query.shape[1]
    width = w_v.shape[0]
    pairs, lines, chunk = keep_out.shape
    step = pl.program_id(0)
    copy = pltpu.make_async_copy(x_hbm, x, sem)

    @pl.when(step == 0)
    def _():
        copy.start()
        key_acc[...] = jnp.zeros_like(key_acc)
        c_acc[...] = jnp.zeros_like(c_acc)

    lane = lax.broadcasted_iota(jnp.int32, (rows, LANES), 1)
    stats = stat[...]
    here = pl.ds(pl.multiple_of(step * rows, rows), rows)
    for h in range(heads):
        p, s = h // 2, h % 2
        zeta = stats[:, h : h + 1]
        scaled = e[h, here, :].astype(f32) * (stats[:, heads + h : heads + h + 1] * grad[...])
        c_acc[h : h + 1, :] += jnp.sum(scaled, axis=0, keepdims=True)
        centred = (scaled * (z[pl.ds(table[0] * heads + h, 1), :] - zeta)).astype(bf16)
        head = query[:, p * LANES : (p + 1) * LANES]
        head = jnp.where((lane >= half) == (s == 1), head, jnp.zeros_like(head))
        key_acc[p * LANES : (p + 1) * LANES, :] += contract(head, centred, ((0,), (0,)))

    @pl.when(step == pl.num_programs(0) - 1)
    def _():
        copy.wait()
        c = c_acc[...]
        high = c.astype(bf16).astype(f32)
        parts = jnp.concatenate([high[:heads], (c - high)[:heads]], axis=0)
        extra = keys_out.shape[0] - own - 2 * heads
        parts = jnp.concatenate([parts, jnp.zeros((extra, total), f32)], axis=0)
        keys_out[:own] = key_acc[...].astype(bf16)
        keys_out[own:] = parts.astype(bf16)
        out = jnp.dot(keys_out[...], x[:, :width], preferred_element_type=f32)
        mass = out[own : own + heads] + out[own + heads : own + 2 * heads]
        high = mass.astype(bf16).astype(f32)
        tops = jnp.concatenate([high, mass - high], axis=0)
        values = jnp.dot(tops.astype(bf16), w_v[...], preferred_element_type=f32)
        values = values[:heads] + values[heads:]
        head = lax.broadcasted_iota(jnp.int32, (heads, own), 1) // half
        index = lax.broadcasted_iota(jnp.int32, (heads, own), 0)
        value = jnp.sum(jnp.where(head == index, values, 0.0), axis=0, keepdims=True)
        count = own // chunk
        cuts = [value[:, t * chunk : (t + 1) * chunk] for t in range(count)]
        fill = lines - own - heads - count
        cuts.append(jnp.zeros((fill, chunk), f32))
        wide_index = table[at_wide]
        odd = wide_index % 2 == 1

        def block(w):
            at = slice(w * chunk, (w + 1) * chunk)
            return out[:own, at], jnp.concatenate([mass[:, at]] + cuts, axis=0)

        for t in range(pairs):
            even, other = block(2 * t), block(2 * t + 1)
            place = jnp.bitwise_xor(t, wide_index // 2)
            for target, first in ((keep_out, False), (send_out, True)):
                top = jnp.where(odd != first, other[0], even[0])
                rest = jnp.where(odd != first, other[1], even[1])
                target[place, :own] = top.astype(bf16)
                target[place, own:] = rest.astype(bf16)


def query_rows_kernel(table, *refs, narrow):
    blocks = refs[:narrow]
    w_q, out = refs[narrow:]
    step = pl.program_id(0)
    for m in range(narrow):

        @pl.when(step == m)
        def _():
            term = contract(blocks[m][...], w_q[...], ((1,), (1,)))
            out[...] = term if m == 0 else out[...] + term


def tail_kernel(table, *refs, narrow, heads):
    keys = refs[:narrow]
    w_k, query_rows, turned, source, incoming, grad, gain, score, out, acc, cs = refs[narrow:]
    own = w_k.shape[1]
    count, piece, width = out.shape
    scale = (LANES // 2) ** -0.5
    step = pl.program_id(0)
    for m in range(narrow):

        @pl.when(step == m)
        def _():
            term = contract(keys[m][:own], w_k[...], ((0,), (1,)))
            acc[...] = term if m == 0 else acc[...] + term
            mass = keys[m][own:].astype(f32)
            for h in range(heads):
                cs[pl.ds(table[m] * heads + h, 1), :] = mass[h : h + 1] + mass[heads + h : heads + h + 1]

    @pl.when(step == narrow - 1)
    def _():
        mass = cs[...]
        high = mass.astype(bf16).astype(f32)
        mass = jnp.concatenate([high, mass - high, high], axis=0).astype(bf16)
        values_part = contract(mass, turned[...], ((0,), (0,)))
        acc[...] += values_part + query_rows[...] * (grad[...] * scale)
        for c in range(count):
            part = pl.ds(c * piece, piece)
            scaled = acc[part, :] * gain[...]
            values = incoming[source[0, c], :, :width].astype(f32)
            inv = lax.rsqrt(jnp.mean(values * values, axis=1, keepdims=True) + epsilon)
            mean = jnp.mean(scaled * values, axis=1, keepdims=True)
            sums = grad[part, :] * score[...] + inv * scaled - values * (inv * inv * inv * mean)
            out[source[0, c]] = sums.astype(bf16)


def body(rows, grades, block_dest, block_source, lengths, gain, w_qkv, w_out, w_score):
    wide = lax.axis_size("wide")
    narrow = lax.axis_size("narrow")
    wide_index = lax.axis_index("wide")
    narrow_index = lax.axis_index("narrow")
    local, width = rows.shape
    lists = lengths.shape[1]
    piece = local // wide
    head_size = width // HEADS
    heads = HEADS // narrow
    own = heads * head_size
    total = local * narrow
    chunk = width // wide
    order = jnp.bitwise_xor(narrow_index, jnp.arange(narrow, dtype=jnp.int32))
    bounds = jnp.cumsum(lax.dynamic_index_in_dim(lengths, wide_index, 0, keepdims=False))
    table = jnp.concatenate([order, bounds.astype(jnp.int32), wide_index[None].astype(jnp.int32)])
    gain_row, score_row = gain[None, :], w_score[None, :]

    def swap(values, m):
        return lax.ppermute(values, "narrow", [(i, i ^ m) for i in range(narrow)])

    def across(values):
        return lax.all_to_all(values, "wide", split_axis=0, concat_axis=0, tiled=True)

    def spread(values):
        held = [values] + [None] * (narrow - 1)
        for m in range(1, narrow):
            top = 1 << (m.bit_length() - 1)
            held[m] = swap(held[m ^ top], top) if m == top else None
        for m in range(1, narrow):
            if held[m] is None:
                top = 1 << (m.bit_length() - 1)
                held[m] = swap(held[top], m ^ top)
        return held

    def shape(*dims, dtype=f32):
        return jax.ShapeDtypeStruct(dims, dtype)

    w_qkv = stay(w_qkv)

    outgoing = call(
        pack_kernel, shape(wide, piece, width + LANES, dtype=bf16), [smem(), vmem(), vmem()]
    )(block_dest, stay(rows.reshape(wide, piece, width)), stay(grades[None, :]))
    incoming = across(outgoing)

    u, g_turned, g_proj = call(
        prepare_kernel,
        (shape(width, 1), shape(3 * HEADS, width, dtype=bf16), shape(width, LANES, dtype=bf16)),
        [pl.BlockSpec((width, width), lambda i: (0, 2)), whole((width, width)), whole((1, width))],
        work=10**9,
        room=24,
        grid=(1,),
        out_specs=(whole((width, 1)), whole((3 * HEADS, width)), whole((width, LANES))),
    )(w_qkv, w_out, score_row)

    normx = call(
        norm_kernel,
        shape(wide, piece, width + LANES, dtype=bf16),
        [smem(), smem(), vmem(), vmem(), vmem(), pl.BlockSpec(memory_space=pl.ANY)],
    )(block_source, table[None, :], near(incoming), gain_row, score_row, g_proj)
    blocks = spread(normx.reshape(local, width + LANES))

    row_block = lambda columns: pl.BlockSpec((local, columns), lambda i, t: (i, 0))
    key, e, queries, x, stat, part, z, lines = indexed(
        lambda *refs: forward_kernel(*refs, narrow=narrow, lists=lists),
        (
            shape(total, own, dtype=bf16),
            shape(heads, total, total, dtype=bf16),
            shape(total, own, dtype=bf16),
            shape(total, width + LANES, dtype=bf16),
            shape(total, LANES),
            shape(1, total),
            shape(HEADS, total),
            shape(8, total),
        ),
        [whole((local, width + LANES))] + [vmem()] * (narrow - 1)
        + [
            pl.BlockSpec((width, own), lambda i, t: (0, t[0])),
            pl.BlockSpec((width, own), lambda i, t: (0, narrow + t[0])),
            whole((width, LANES)),
        ],
        (
            whole((total, own)),
            pl.BlockSpec((heads, local, total), lambda i, t: (0, i, 0)),
            row_block(own),
            row_block(width + LANES),
            row_block(LANES),
            pl.BlockSpec((1, local), lambda i, t: (0, i)),
            whole((HEADS, total)),
            whole((8, total)),
        ),
        (narrow,),
        [
            pltpu.VMEM((total, width + LANES), bf16),
            pltpu.VMEM((total, own), bf16),
            pltpu.VMEM((heads // 2, total, 2 * LANES), bf16),
            pltpu.VMEM((HEADS, total), f32),
        ],
        work=4 * 10**9,
        room=28,
    )(table, blocks[0], *map(near, blocks[1:]), w_qkv, w_qkv, g_proj)

    partials = [part] + [swap(part, m) for m in range(1, narrow)]
    a = indexed(
        center_kernel,
        shape(total, own, dtype=bf16),
        [vmem(), row_block(LANES), whole((total, own)), whole((HEADS, total))],
        row_block(own),
        (narrow,),
        work=2 * 10**9,
        room=10,
    )(table, near(e), stat, key, z)
    a_rows = [a[:local]] + [swap(a[m * local : (m + 1) * local], m) for m in range(1, narrow)]

    grad, gq = indexed(
        lambda *refs: score_kernel(*refs, narrow=narrow),
        (shape(total, 1), shape(wide, own, chunk, dtype=bf16)),
        [whole((1, total))] + [vmem()] * (narrow - 1) + [whole((8, total)), row_block(width + LANES), row_block(own)],
        (row_block(1), whole((wide, own, chunk))),
        (narrow,),
        [pltpu.VMEM((8, total), f32), pltpu.VMEM((own, width), f32)],
        work=2 * 10**9,
        room=14,
    )(table, partials[0], *map(near, partials[1:]), lines, x, a)
    terms_q = across(gq)

    count_v = own // chunk
    lines_k = -(-(own + heads + count_v) // 16) * 16
    lines_c = -(-(own + 2 * heads) // 16) * 16
    keys, keep, send = indexed(
        lambda *refs: key_kernel(*refs, at_wide=narrow + lists),
        (shape(lines_c, total, dtype=bf16),) + (shape(wide // 2, lines_k, chunk, dtype=bf16),) * 2,
        [
            vmem(),
            row_block(LANES),
            row_block(own),
            whole((HEADS, total)),
            row_block(1),
            pl.BlockSpec((width, own), lambda i, t: (0, 2 * narrow + t[0])),
            pl.BlockSpec(memory_space=pl.ANY),
        ],
        (whole((lines_c, total)),) + (whole((wide // 2, lines_k, chunk)),) * 2,
        (narrow,),
        [
            pltpu.VMEM((total, width + LANES), bf16),
            pltpu.VMEM((own, total), f32),
            pltpu.VMEM((8, total), f32),
            pltpu.SemaphoreType.DMA,
        ],
        work=4 * 10**9,
        room=22,
    )(table, near(e), stat, queries, z, grad, w_qkv, x)

    k_rows = [keys[:, :local]]
    k_rows += [swap(keys[:, m * local : (m + 1) * local], m) for m in range(1, narrow)]
    step = 1
    while True:
        received = lax.ppermute(send, "wide", [(i, i ^ step) for i in range(wide)])
        sum_k = keep.astype(f32) + received.astype(f32)
        step *= 2
        if step == wide:
            break
        cut = sum_k.astype(bf16).reshape(-1, 2, lines_k, chunk)
        keep, send = cut[:, 0], cut[:, 1]
    sum_k = sum_k[0].astype(bf16)

    query_rows = indexed(
        lambda *refs: query_rows_kernel(*refs, narrow=narrow),
        shape(local, width),
        [vmem()] * narrow + [pl.BlockSpec((width, own), lambda i, t: (0, t[i]))],
        whole((local, width)),
        (narrow,),
        work=10**9,
        room=8,
    )(table, *map(near, a_rows), w_qkv)
    returning = indexed(
        lambda *refs: tail_kernel(*refs, narrow=narrow, heads=heads),
        shape(wide, piece, width, dtype=bf16),
        [vmem()] * narrow
        + [
            pl.BlockSpec((width, own), lambda i, t: (0, narrow + t[i])),
            vmem(),
            whole((3 * HEADS, width)),
            smem(),
            vmem(),
            whole((local, 1)),
            whole((1, width)),
            whole((1, width)),
        ],
        whole((wide, piece, width)),
        (narrow,),
        [pltpu.VMEM((local, width), f32), pltpu.VMEM((HEADS, local), f32)],
        work=10**9,
        room=10,
    )(
        table, *map(near, k_rows), w_qkv, near(query_rows), g_turned, block_source, near(incoming), grad, gain_row, score_row
    )
    arrived = across(returning)
    grad_rows = arrived[block_dest[0]].reshape(local, width)

    sum_q = jnp.sum(terms_q.astype(f32), axis=0)
    q_cols = jnp.stack(spread(sum_q.astype(bf16)))[order].reshape(width, chunk)
    gathered = jnp.stack(spread(sum_k))[order]
    k_cols = gathered[:, :own].reshape(width, chunk)
    m_all = gathered[:, own : own + heads].astype(f32)
    m_rows = jnp.broadcast_to(m_all.reshape(HEADS, 1, chunk), (HEADS, head_size, chunk))
    v_cols = (m_rows.reshape(width, chunk) * u).astype(bf16)
    v_all = gathered[:, own + heads : own + heads + count_v].astype(f32)
    v_all = v_all.reshape(width)
    columns = 3 * width // (wide * narrow)
    full = jnp.concatenate([q_cols, k_cols, v_cols], axis=0).reshape(wide, narrow, columns, chunk)
    mine = lax.dynamic_index_in_dim(full, narrow_index, 1, keepdims=False)
    parts = across(mine)
    grad_qkv = parts.astype(f32).transpose(0, 2, 1).reshape(width, columns)
    out_columns = width // (wide * narrow)
    place = (wide_index * narrow + narrow_index) * out_columns
    grad_out = v_all[:, None] * lax.dynamic_slice_in_dim(w_score, place, out_columns)[None, :]
    return (grad_rows, grad_qkv, grad_out)


def solution(mesh):
    both = ("wide", "narrow")
    placed = (P(both, None), P(both), P(both, None), P(both, None), P(), P(), P(), P(), P())
    return jax.shard_map(
        body,
        mesh=mesh,
        in_specs=placed,
        out_specs=(P(both, None), P(None, both), P(None, both)),
        check_vma=False,
    )
```

```python
import jax
import jax.numpy as jnp
from jax import lax
from jax.experimental import pallas as pl
from jax.experimental.pallas import tpu as pltpu
from jax.sharding import PartitionSpec as P


HEADS = 16
LANES = 128
epsilon = 1e-06
loss_scale = 64.0
log2e = 1.4426950408889634
far = 2.0**100
bf16 = jnp.bfloat16
f32 = jnp.float32


def vmem():
    return pl.BlockSpec(memory_space=pltpu.VMEM)


def smem():
    return pl.BlockSpec(memory_space=pltpu.SMEM)


def whole(shape):
    return pl.BlockSpec(shape, lambda *_: (0,) * len(shape))


def call(kernel, shapes, specs, work=0, room=8, **more):
    params = pltpu.CompilerParams(vmem_limit_bytes=room * 2**20)
    cost = pl.CostEstimate(flops=work, transcendentals=0, bytes_accessed=0)
    return pl.pallas_call(
        kernel, out_shape=shapes, in_specs=specs, compiler_params=params, cost_estimate=cost, **more
    )


def indexed(kernel, shapes, specs, out_specs, grid, scratch=(), work=0, room=8):
    params = pltpu.CompilerParams(vmem_limit_bytes=room * 2**20)
    cost = pl.CostEstimate(flops=work, transcendentals=0, bytes_accessed=0)
    spec = pltpu.PrefetchScalarGridSpec(
        num_scalar_prefetch=1, grid=grid, in_specs=specs, out_specs=out_specs, scratch_shapes=scratch
    )
    return pl.pallas_call(
        kernel, out_shape=shapes, grid_spec=spec, compiler_params=params, cost_estimate=cost
    )


def near(values):
    return pltpu.with_memory_space_constraint(values, pltpu.VMEM)


def stay(values):
    return pltpu.with_memory_space_constraint(values, pltpu.HBM)


def contract(left, right, dims, **more):
    return lax.dot_general(left, right, (dims, ((), ())), preferred_element_type=f32, **more)


def prepare_kernel(w_v, w_out, score, u_out, turned_out, proj_out):
    width = w_v.shape[0]
    half = LANES // 2
    u = jnp.sum(w_out[...].astype(f32) * score[...], axis=1, keepdims=True)
    u_out[...] = u
    high = u.astype(bf16).astype(f32)
    lane = lax.broadcasted_iota(jnp.int32, (width, LANES), 1)
    head = lax.broadcasted_iota(jnp.int32, (width, LANES), 0) // (width // HEADS)
    columns = jnp.where(lane == head, high, 0.0)
    columns = jnp.where(lane == half + head, u - high, columns).astype(bf16)
    g = jnp.dot(w_v[...], columns, preferred_element_type=f32)
    g = g + pltpu.roll(g, half, axis=1)
    high = g.astype(bf16).astype(f32)
    tops, rests = high.T[:HEADS], (g - high).T[:HEADS]
    turned_out[...] = jnp.concatenate([tops, tops, rests], axis=0).astype(bf16)
    proj_out[...] = jnp.where(lane < half, high, g - high).astype(bf16)


def pack_kernel(dest, rows, grades, out):
    count, piece, width = rows.shape
    total = grades.shape[1]
    row = lax.broadcasted_iota(jnp.int32, (piece, total), 0)
    lane = lax.broadcasted_iota(jnp.int32, (piece, total), 1)
    line = grades[...].astype(f32)
    for b in range(count):
        grade = jnp.sum(jnp.where(lane == row + b * piece, line, 0.0), axis=1, keepdims=True)
        out[dest[0, b], :, :width] = rows[b]
        out[dest[0, b], :, width:] = jnp.broadcast_to(grade, (piece, LANES)).astype(bf16)


def norm_kernel(source, table, incoming, gain, score, ready, out, info_out, held):
    count, piece, wide = incoming.shape
    width = wide - LANES
    lane = lax.broadcasted_iota(jnp.int32, (piece, LANES), 1)
    for c in range(count):
        block = incoming[source[0, c]]
        values = block[:, :width].astype(f32)
        inverse = lax.rsqrt(jnp.mean(values * values, axis=1, keepdims=True) + epsilon)
        out[c] = (values * inverse * gain[...]).astype(bf16)
        base = jnp.sum(values * score[...], axis=1, keepdims=True)
        grades = block[:, width:].astype(f32)
        held[c * piece : (c + 1) * piece, :] = jnp.where(lane == 0, base, jnp.exp2(grades))
    info_out[...] = held[...].T[:8]


def list_of(table, narrow, lists, first, shape, axis):
    position = lax.broadcasted_iota(jnp.int32, shape, axis) + first
    found = jnp.zeros(shape, jnp.int32)
    for s in range(lists):
        found = found + (position >= table[narrow + s]).astype(jnp.int32)
    return found


def project(block, w_q, w_k, g):
    half = LANES // 2
    query = jnp.dot(block, w_q, preferred_element_type=f32) * half**-0.5
    key = jnp.dot(block, w_k, preferred_element_type=f32)
    turned = jnp.dot(block, g, preferred_element_type=f32).T
    return query.astype(bf16), key.astype(bf16), turned[:HEADS] + turned[half : half + HEADS]


def early_kernel(table, first, second, w_q, w_k, g, w_out, q_out, k_out, z_out):
    local = first.shape[0]
    own = w_q.shape[1]
    w_out[:, :own] = w_q[...]
    w_out[:, own:] = w_k[...]
    for m, block in enumerate((first, second)):
        rows = slice(m * local, (m + 1) * local)
        q_out[rows, :], k_out[rows, :], z_out[:, rows] = project(block[...], w_q[...], w_k[...], g[...])


def forward_kernel(table, *refs, narrow, lists):
    blocks, infos = refs[:narrow], refs[narrow : 2 * narrow]
    refs = refs[2 * narrow :]
    w, q_early, k_early, z_early, g, k_out, e_out, q_out, x_out, stat_out, part_out, z_out, lines_out = refs[:13]
    qs, kx, zt = refs[13:]
    local = blocks[0].shape[0]
    own = q_early.shape[1]
    heads = e_out.shape[0]
    half = LANES // 2
    step = pl.program_id(0)

    @pl.when(step == 0)
    def _():
        lane = lax.broadcasted_iota(jnp.int32, (local, LANES), 1)
        for m in range(narrow):
            rows = pl.ds(m * local, local)
            x_out[rows, :] = blocks[m][...]
            if m < 2:
                query, keys, turned = q_early[rows, :], k_early[rows, :], z_early[:, rows]
            else:
                query, keys, turned = project(blocks[m][...], w[:, :own], w[:, own:], g[...])
            qs[rows, :] = query
            k_out[rows, :] = keys
            zt[:, rows] = turned
            segment = list_of(table, narrow, lists, table[m] * local, (local, LANES), 0)
            away = jnp.where(lane == segment, 0.0, -far).astype(bf16)
            for p in range(heads // 2):
                kx[p, rows, :LANES] = keys[:, p * LANES : (p + 1) * LANES]
                kx[p, rows, LANES:] = away
            lines_out[:, rows] = infos[m][...]
            lines_out[2:3, rows] = list_of(table, narrow, lists, table[m] * local, (1, local), 1).astype(f32)
        z_out[...] = zt[...]

    at = pl.ds(pl.multiple_of(step * local, local), local)
    query = qs[at, :]
    q_out[...] = query
    lane = lax.broadcasted_iota(jnp.int32, (local, LANES), 1)
    segment = list_of(table, narrow, lists, table[step] * local, (local, LANES), 0)
    mine = (lane == segment).astype(f32).astype(bf16)
    stats = jnp.zeros((local, LANES), f32)
    zsum = jnp.zeros((local, 1), f32)
    for p in range(heads // 2):
        for s in range(2):
            h = 2 * p + s
            own = query[:, p * LANES : (p + 1) * LANES]
            own = jnp.where((lane >= half) == (s == 1), own, jnp.zeros_like(own))
            logits = contract(jnp.concatenate([own, mine], axis=1), kx[p], ((1,), (1,)))
            weights = jnp.exp2(logits * log2e)
            e_out[h] = weights.astype(bf16)
            zrow = zt[pl.ds(table[0] * heads + h, 1), :]
            inverse = 1.0 / jnp.sum(weights, axis=1, keepdims=True)
            zeta = jnp.sum(weights * zrow, axis=1, keepdims=True) * inverse
            stats = jnp.where(lane == h, zeta, stats)
            stats = jnp.where(lane == heads + h, inverse, stats)
            zsum = zsum + zeta
    stat_out[...] = stats
    part_out[...] = jnp.broadcast_to(zsum, (local, LANES)).T[:1]


def center_kernel(table, e, stat, key, z, a_out):
    heads = e.shape[0]
    rows = stat.shape[0]
    half = LANES // 2
    here = pl.ds(pl.multiple_of(pl.program_id(0) * rows, rows), rows)
    lane = lax.broadcasted_iota(jnp.int32, (rows, LANES), 1)
    stats = stat[...]
    for p in range(heads // 2):
        at = slice(p * LANES, (p + 1) * LANES)
        parts = []
        for h in (2 * p, 2 * p + 1):
            zrow = z[pl.ds(table[0] * heads + h, 1), :]
            centred = (e[h, here, :].astype(f32) * (zrow - stats[:, h : h + 1])).astype(bf16)
            part = jnp.dot(centred, key[:, at], preferred_element_type=f32)
            parts.append(part * stats[:, heads + h : heads + h + 1])
        a_out[:, at] = jnp.where(lane >= half, parts[1], parts[0]).astype(bf16)


def halves(blocks, pairs, wide_index, keep_out, send_out):
    odd = wide_index % 2 == 1
    for t in range(pairs):
        even, other = blocks(2 * t), blocks(2 * t + 1)
        place = jnp.bitwise_xor(t, wide_index // 2)
        keep_out[place] = jnp.where(odd, other, even).astype(bf16)
        send_out[place] = jnp.where(odd, even, other).astype(bf16)


def score_kernel(table, *refs, narrow, lists):
    partials = refs[:narrow]
    given, x, a, grad_out, keep_out, send_out, lines, acc = refs[narrow:]
    local, _ = a.shape
    width = x.shape[1]
    scale = (LANES // 2) ** -0.5
    pairs, _, chunk = keep_out.shape
    step = pl.program_id(0)

    @pl.when(step == 0)
    def _():
        acc[...] = jnp.zeros_like(acc)
        lines[...] = given[...]
        for m in range(narrow):
            rows = pl.ds(m * local, local)
            summed = given[0:1, rows]
            for d in range(narrow):
                summed = summed + partials[d][:, (m ^ d) * local : ((m ^ d) + 1) * local]
            lines[0:1, rows] = summed

    at = pl.ds(pl.multiple_of(step * local, local), local)
    turned = jnp.concatenate([lines[:, at]] * (LANES // 8), axis=0).T
    same = turned[:, 2:3] == lines[2:3, :]
    gains = lines[1:2, :]
    spread = gains - turned[:, 1:2]
    margin = turned[:, 0:1] - lines[0:1, :]
    margin = jnp.where(spread > 0.0, margin, -margin)
    pulls = spread / (1.0 + jnp.exp(-margin))
    pulls = jnp.sum(jnp.where(same, pulls, 0.0), axis=1, keepdims=True)
    norm = jnp.sum(jnp.where(same, gains, 0.0), axis=1, keepdims=True)
    grad = loss_scale * pulls / norm
    grad_out[...] = grad
    query = (a[...].astype(f32) * (grad * scale)).astype(bf16)
    acc[...] += contract(query, x[:, :width], ((0,), (0,)))

    @pl.when(step == pl.num_programs(0) - 1)
    def _():
        cut = lambda w: acc[:, w * chunk : (w + 1) * chunk]
        halves(cut, pairs, table[narrow + lists], keep_out, send_out)


def key_kernel(table, e, stat, query, z, grad, w_v, x_hbm, keys_out, keep_out, send_out, x, key_acc, c_acc, sem, at_wide):
    heads, total, _ = e.shape
    rows = query.shape[0]
    half = LANES // 2
    own = query.shape[1]
    width = w_v.shape[0]
    pairs, lines, chunk = keep_out.shape
    step = pl.program_id(0)
    copy = pltpu.make_async_copy(x_hbm, x, sem)

    @pl.when(step == 0)
    def _():
        copy.start()
        key_acc[...] = jnp.zeros_like(key_acc)
        c_acc[...] = jnp.zeros_like(c_acc)

    lane = lax.broadcasted_iota(jnp.int32, (rows, LANES), 1)
    stats = stat[...]
    here = pl.ds(pl.multiple_of(step * rows, rows), rows)
    for h in range(heads):
        p, s = h // 2, h % 2
        zeta = stats[:, h : h + 1]
        scaled = e[h, here, :].astype(f32) * (stats[:, heads + h : heads + h + 1] * grad[...])
        c_acc[h : h + 1, :] += jnp.sum(scaled, axis=0, keepdims=True)
        centred = (scaled * (z[pl.ds(table[0] * heads + h, 1), :] - zeta)).astype(bf16)
        head = query[:, p * LANES : (p + 1) * LANES]
        head = jnp.where((lane >= half) == (s == 1), head, jnp.zeros_like(head))
        key_acc[p * LANES : (p + 1) * LANES, :] += contract(head, centred, ((0,), (0,)))

    @pl.when(step == pl.num_programs(0) - 1)
    def _():
        copy.wait()
        c = c_acc[...]
        high = c.astype(bf16).astype(f32)
        parts = jnp.concatenate([high[:heads], (c - high)[:heads]], axis=0)
        extra = keys_out.shape[0] - own - 2 * heads
        parts = jnp.concatenate([parts, jnp.zeros((extra, total), f32)], axis=0)
        keys_out[:own] = key_acc[...].astype(bf16)
        keys_out[own:] = parts.astype(bf16)
        out = jnp.dot(keys_out[...], x[:, :width], preferred_element_type=f32)
        mass = out[own : own + heads] + out[own + heads : own + 2 * heads]
        high = mass.astype(bf16).astype(f32)
        tops = jnp.concatenate([high, mass - high], axis=0)
        values = jnp.dot(tops.astype(bf16), w_v[...], preferred_element_type=f32)
        values = values[:heads] + values[heads:]
        head = lax.broadcasted_iota(jnp.int32, (heads, own), 1) // half
        index = lax.broadcasted_iota(jnp.int32, (heads, own), 0)
        value = jnp.sum(jnp.where(head == index, values, 0.0), axis=0, keepdims=True)
        count = own // chunk
        cuts = [value[:, t * chunk : (t + 1) * chunk] for t in range(count)]
        fill = lines - own - heads - count
        cuts.append(jnp.zeros((fill, chunk), f32))

        def block(w):
            at = slice(w * chunk, (w + 1) * chunk)
            return jnp.concatenate([out[:own, at], mass[:, at]] + cuts, axis=0)

        halves(block, pairs, table[at_wide], keep_out, send_out)


def fetch(table, w, buffer, sems, first):
    narrow, _, own = buffer.shape
    copies = []
    for m in range(narrow):
        at = pl.ds(pl.multiple_of((table[m] + first) * own, own), own)
        copies.append(pltpu.make_async_copy(w.at[:, at], buffer.at[m], sems.at[m]))
        copies[m].start()
    return copies


def query_rows_kernel(table, *refs):
    *blocks, w, out, buffer, sems = refs
    copies = fetch(table, w, buffer, sems, 0)
    for m, block in enumerate(blocks):
        copies[m].wait()
        term = contract(block[...], buffer[m], ((1,), (1,)))
        out[...] = term if m == 0 else out[...] + term


def tail_kernel(table, *refs, narrow, heads):
    keys = refs[:narrow]
    w, query_rows, turned, source, incoming, grad, gain, score, out, acc, cs, buffer, sems = refs[narrow:]
    copies = fetch(table, w, buffer, sems, narrow)
    count, piece, width = out.shape
    own = width // narrow
    scale = (LANES // 2) ** -0.5
    acc[...] = query_rows[...] * (grad[...] * scale)
    for m in range(narrow):
        copies[m].wait()
        acc[...] += contract(keys[m][:own], buffer[m], ((0,), (1,)))
        mass = keys[m][own:].astype(f32)
        for h in range(heads):
            cs[pl.ds(table[m] * heads + h, 1), :] = mass[h : h + 1] + mass[heads + h : heads + h + 1]
    mass = cs[...]
    high = mass.astype(bf16).astype(f32)
    mass = jnp.concatenate([high, mass - high, high], axis=0).astype(bf16)
    acc[...] += contract(mass, turned[...], ((0,), (0,)))
    for c in range(count):
        part = pl.ds(c * piece, piece)
        scaled = acc[part, :] * gain[...]
        values = incoming[source[0, c], :, :width].astype(f32)
        inv = lax.rsqrt(jnp.mean(values * values, axis=1, keepdims=True) + epsilon)
        mean = jnp.mean(scaled * values, axis=1, keepdims=True)
        sums = grad[part, :] * score[...] + inv * scaled - values * (inv * inv * inv * mean)
        out[source[0, c]] = sums.astype(bf16)


def body(rows, grades, block_dest, block_source, lengths, gain, w_qkv, w_out, w_score):
    wide = lax.axis_size("wide")
    narrow = lax.axis_size("narrow")
    wide_index = lax.axis_index("wide")
    narrow_index = lax.axis_index("narrow")
    local, width = rows.shape
    lists = lengths.shape[1]
    piece = local // wide
    head_size = width // HEADS
    heads = HEADS // narrow
    own = heads * head_size
    total = local * narrow
    chunk = width // wide
    order = jnp.bitwise_xor(narrow_index, jnp.arange(narrow, dtype=jnp.int32))
    bounds = jnp.cumsum(lax.dynamic_index_in_dim(lengths, wide_index, 0, keepdims=False))
    table = jnp.concatenate([order, bounds.astype(jnp.int32), wide_index[None].astype(jnp.int32)])
    gain_row, score_row = gain[None, :], w_score[None, :]

    def swap(values, m):
        return lax.ppermute(values, "narrow", [(i, i ^ m) for i in range(narrow)])

    def across(values):
        return lax.all_to_all(values, "wide", split_axis=0, concat_axis=0, tiled=True)

    def spread(values):
        held = [values]
        for m in range(1, narrow):
            top = 1 << (m.bit_length() - 1)
            near_by = m ^ top
            held.append(swap(values, m) if near_by == 0 else None)
        for m in range(1, narrow):
            if held[m] is None:
                top = 1 << (m.bit_length() - 1)
                held[m] = swap(held[top], m ^ top)
        return held

    def shape(*dims, dtype=f32):
        return jax.ShapeDtypeStruct(dims, dtype)

    outgoing = call(
        pack_kernel, shape(wide, piece, width + LANES, dtype=bf16), [smem(), vmem(), vmem()]
    )(stay(block_dest), stay(rows.reshape(wide, piece, width)), stay(grades[None, :]))
    incoming = across(outgoing)

    u, g_turned, g_proj = call(
        prepare_kernel,
        (shape(width, 1), shape(3 * HEADS, width, dtype=bf16), shape(width, LANES, dtype=bf16)),
        [pl.BlockSpec((width, width), lambda i: (0, 2)), whole((width, width)), whole((1, width))],
        work=10**9,
        room=24,
        grid=(1,),
        out_specs=(whole((width, 1)), whole((3 * HEADS, width)), whole((width, LANES))),
    )(stay(w_qkv), w_out, score_row)

    normed, info = call(
        norm_kernel,
        (shape(wide, piece, width, dtype=bf16), shape(8, local)),
        [smem(), smem(), vmem(), vmem(), vmem(), pl.BlockSpec(memory_space=pl.ANY)],
        scratch_shapes=[pltpu.VMEM((local, LANES), f32)],
    )(block_source, table[None, :], near(incoming), gain_row, score_row, g_proj)
    blocks = spread(normed.reshape(local, width))
    infos = [info] + [swap(info, m) for m in range(1, narrow)]

    row_block = lambda columns: pl.BlockSpec((local, columns), lambda i, t: (i, 0))
    early = indexed(
        early_kernel,
        (
            shape(width, 2 * own, dtype=bf16),
            shape(2 * local, own, dtype=bf16),
            shape(2 * local, own, dtype=bf16),
            shape(HEADS, 2 * local),
        ),
        [
            vmem(),
            vmem(),
            pl.BlockSpec((width, own), lambda i, t: (0, t[0])),
            pl.BlockSpec((width, own), lambda i, t: (0, narrow + t[0])),
            vmem(),
        ],
        (vmem(),) * 4,
        (1,),
        work=10**9,
        room=10,
    )(table, near(blocks[0]), near(blocks[1]), stay(w_qkv), stay(w_qkv), near(g_proj))
    key, e, queries, x, stat, part, z, lines = indexed(
        lambda *refs: forward_kernel(*refs, narrow=narrow, lists=lists),
        (
            shape(total, own, dtype=bf16),
            shape(heads, total, total, dtype=bf16),
            shape(total, own, dtype=bf16),
            shape(total, width, dtype=bf16),
            shape(total, LANES),
            shape(1, total),
            shape(HEADS, total),
            shape(8, total),
        ),
        [vmem()] * (2 * narrow + 5),
        (
            whole((total, own)),
            pl.BlockSpec((heads, local, total), lambda i, t: (0, i, 0)),
            row_block(own),
            vmem(),
            row_block(LANES),
            pl.BlockSpec((1, local), lambda i, t: (0, i)),
            whole((HEADS, total)),
            whole((8, total)),
        ),
        (narrow,),
        [
            pltpu.VMEM((total, own), bf16),
            pltpu.VMEM((heads // 2, total, 2 * LANES), bf16),
            pltpu.VMEM((HEADS, total), f32),
        ],
        work=4 * 10**9,
        room=28,
    )(table, *map(near, [*blocks, *infos, *early, g_proj]))

    partials = [part] + [swap(part, m) for m in range(1, narrow)]
    a = indexed(
        center_kernel,
        shape(total, own, dtype=bf16),
        [vmem(), row_block(LANES), whole((total, own)), whole((HEADS, total))],
        row_block(own),
        (narrow,),
        work=2 * 10**9,
        room=10,
    )(table, near(e), stat, key, z)
    a_rows = [a[:local]] + [swap(a[m * local : (m + 1) * local], m) for m in range(1, narrow)]

    grad, keep_q, send_q = indexed(
        lambda *refs: score_kernel(*refs, narrow=narrow, lists=lists),
        (shape(total, 1),) + (shape(wide // 2, own, chunk, dtype=bf16),) * 2,
        [whole((1, total))] + [vmem()] * (narrow - 1) + [whole((8, total)), row_block(width), row_block(own)],
        (row_block(1),) + (whole((wide // 2, own, chunk)),) * 2,
        (narrow,),
        [pltpu.VMEM((8, total), f32), pltpu.VMEM((own, width), f32)],
        work=2 * 10**9,
        room=14,
    )(table, partials[0], *map(near, partials[1:]), lines, x, a)

    def to_partner(values, step):
        return lax.ppermute(values, "wide", [(i, i ^ step) for i in range(wide)])

    def added(kept, received):
        return kept.astype(f32) + received.astype(f32)

    got_q = to_partner(send_q, 1)

    count_v = own // chunk
    lines_k = -(-(own + heads + count_v) // 16) * 16
    lines_c = -(-(own + 2 * heads) // 16) * 16
    keys, keep, send = indexed(
        lambda *refs: key_kernel(*refs, at_wide=narrow + lists),
        (shape(lines_c, total, dtype=bf16),) + (shape(wide // 2, lines_k, chunk, dtype=bf16),) * 2,
        [
            vmem(),
            row_block(LANES),
            row_block(own),
            whole((HEADS, total)),
            row_block(1),
            pl.BlockSpec((width, own), lambda i, t: (0, 2 * narrow + t[0])),
            pl.BlockSpec(memory_space=pl.ANY),
        ],
        (whole((lines_c, total)),) + (whole((wide // 2, lines_k, chunk)),) * 2,
        (narrow,),
        [
            pltpu.VMEM((total, width), bf16),
            pltpu.VMEM((own, total), f32),
            pltpu.VMEM((8, total), f32),
            pltpu.SemaphoreType.DMA,
        ],
        work=4 * 10**9,
        room=22,
    )(table, near(e), stat, queries, z, grad, stay(w_qkv), x)

    k_rows = [keys[:, :local]]
    k_rows += [swap(keys[:, m * local : (m + 1) * local], m) for m in range(1, narrow)]
    got_k = to_partner(send, 1)
    sums = jnp.concatenate([added(keep_q, got_q), added(keep, got_k)], axis=1)
    step = 2
    while step < wide:
        cut = sums.astype(bf16).reshape(-1, 2, own + lines_k, chunk)
        sums = added(cut[:, 0], to_partner(cut[:, 1], step))
        step *= 2
    sums = sums[0].astype(bf16)

    fetched = [pltpu.VMEM((narrow, width, own), bf16), pltpu.SemaphoreType.DMA((narrow,))]
    anywhere = pl.BlockSpec(memory_space=pl.ANY)
    query_rows = indexed(
        query_rows_kernel,
        shape(local, width),
        [vmem()] * narrow + [anywhere],
        vmem(),
        (),
        fetched,
        work=10**9,
    )(table, *map(near, a_rows), stay(w_qkv))
    returning = indexed(
        lambda *refs: tail_kernel(*refs, narrow=narrow, heads=heads),
        shape(wide, piece, width, dtype=bf16),
        [vmem()] * narrow + [anywhere] + [vmem()] * 2 + [smem()] + [vmem()] * 4,
        vmem(),
        (),
        [pltpu.VMEM((local, width), f32), pltpu.VMEM((HEADS, local), f32)] + fetched,
        work=10**9,
        room=10,
    )(
        table, *map(near, k_rows), stay(w_qkv), near(query_rows), g_turned, block_source,
        near(incoming), grad[:local], gain_row, score_row,
    )
    arrived = across(returning)
    grad_rows = arrived[block_dest[0]].reshape(local, width)

    gathered = jnp.stack(spread(sums))[order]
    q_cols = gathered[:, :own].reshape(width, chunk)
    gathered = gathered[:, own:]
    k_cols = gathered[:, :own].reshape(width, chunk)
    m_all = gathered[:, own : own + heads].astype(f32)
    m_rows = jnp.broadcast_to(m_all.reshape(HEADS, 1, chunk), (HEADS, head_size, chunk))
    v_cols = (m_rows.reshape(width, chunk) * u).astype(bf16)
    v_all = gathered[:, own + heads : own + heads + count_v].astype(f32)
    v_all = v_all.reshape(width)
    columns = 3 * width // (wide * narrow)
    full = jnp.concatenate([q_cols, k_cols, v_cols], axis=0).reshape(wide, narrow, columns, chunk)
    mine = lax.dynamic_index_in_dim(full, narrow_index, 1, keepdims=False)
    parts = across(mine)
    grad_qkv = parts.astype(f32).transpose(0, 2, 1).reshape(width, columns)
    out_columns = width // (wide * narrow)
    place = (wide_index * narrow + narrow_index) * out_columns
    grad_out = v_all[:, None] * lax.dynamic_slice_in_dim(w_score, place, out_columns)[None, :]
    return (grad_rows, grad_qkv, grad_out)


def solution(mesh):
    both = ("wide", "narrow")
    placed = (P(both, None), P(both), P(both, None), P(both, None), P(), P(), P(), P(), P())
    return jax.shard_map(
        body,
        mesh=mesh,
        in_specs=placed,
        out_specs=(P(both, None), P(None, both), P(None, both)),
        check_vma=False,
    )
```

```python
import jax
import jax.numpy as jnp
from jax import lax
from jax.experimental import pallas as pl
from jax.experimental.pallas import tpu as pltpu
from jax.sharding import PartitionSpec as P


HEADS = 16
LANES = 128
epsilon = 1e-06
loss_scale = 64.0
log2e = 1.4426950408889634
far = 2.0**100
bf16 = jnp.bfloat16
f32 = jnp.float32


def vmem():
    return pl.BlockSpec(memory_space=pltpu.VMEM)


def smem():
    return pl.BlockSpec(memory_space=pltpu.SMEM)


def whole(shape):
    return pl.BlockSpec(shape, lambda *_: (0,) * len(shape))


def call(kernel, shapes, specs, work=0, room=8, **more):
    params = pltpu.CompilerParams(vmem_limit_bytes=room * 2**20)
    cost = pl.CostEstimate(flops=work, transcendentals=0, bytes_accessed=0)
    return pl.pallas_call(
        kernel, out_shape=shapes, in_specs=specs, compiler_params=params, cost_estimate=cost, **more
    )


def indexed(kernel, shapes, specs, out_specs, grid, scratch=(), work=0, room=8):
    params = pltpu.CompilerParams(vmem_limit_bytes=room * 2**20)
    cost = pl.CostEstimate(flops=work, transcendentals=0, bytes_accessed=0)
    spec = pltpu.PrefetchScalarGridSpec(
        num_scalar_prefetch=1, grid=grid, in_specs=specs, out_specs=out_specs, scratch_shapes=scratch
    )
    return pl.pallas_call(
        kernel, out_shape=shapes, grid_spec=spec, compiler_params=params, cost_estimate=cost
    )


def near(values):
    return pltpu.with_memory_space_constraint(values, pltpu.VMEM)


def stay(values):
    return pltpu.with_memory_space_constraint(values, pltpu.HBM)


def contract(left, right, dims, **more):
    return lax.dot_general(left, right, (dims, ((), ())), preferred_element_type=f32, **more)


def prepare_kernel(w_v, w_out, score, u_out, turned_out, proj_out):
    width = w_v.shape[0]
    half = LANES // 2
    u = jnp.sum(w_out[...].astype(f32) * score[...], axis=1, keepdims=True)
    u_out[...] = u
    high = u.astype(bf16).astype(f32)
    lane = lax.broadcasted_iota(jnp.int32, (width, LANES), 1)
    head = lax.broadcasted_iota(jnp.int32, (width, LANES), 0) // (width // HEADS)
    columns = jnp.where(lane == head, high, 0.0)
    columns = jnp.where(lane == half + head, u - high, columns).astype(bf16)
    g = jnp.dot(w_v[...], columns, preferred_element_type=f32)
    g = g + pltpu.roll(g, half, axis=1)
    high = g.astype(bf16).astype(f32)
    tops, rests = high.T[:HEADS], (g - high).T[:HEADS]
    turned_out[...] = jnp.concatenate([tops, tops, rests], axis=0).astype(bf16)
    proj_out[...] = jnp.where(lane < half, high, g - high).astype(bf16)


def pack_kernel(dest, rows, grades, out):
    count, piece, width = rows.shape
    total = grades.shape[1]
    row = lax.broadcasted_iota(jnp.int32, (piece, total), 0)
    lane = lax.broadcasted_iota(jnp.int32, (piece, total), 1)
    line = grades[...].astype(f32)
    for b in range(count):
        grade = jnp.sum(jnp.where(lane == row + b * piece, line, 0.0), axis=1, keepdims=True)
        out[dest[0, b], :, :width] = rows[b]
        out[dest[0, b], :, width:] = jnp.broadcast_to(grade, (piece, LANES)).astype(bf16)


def norm_kernel(source, table, incoming, gain, score, ready, out, info_out, held):
    count, piece, wide = incoming.shape
    width = wide - LANES
    lane = lax.broadcasted_iota(jnp.int32, (piece, LANES), 1)
    for c in range(count):
        block = incoming[source[0, c]]
        values = block[:, :width].astype(f32)
        inverse = lax.rsqrt(jnp.mean(values * values, axis=1, keepdims=True) + epsilon)
        out[c] = (values * inverse * gain[...]).astype(bf16)
        base = jnp.sum(values * score[...], axis=1, keepdims=True)
        grades = block[:, width:].astype(f32)
        held[c * piece : (c + 1) * piece, :] = jnp.where(lane == 0, base, jnp.exp2(grades))
    info_out[...] = held[...].T[:8]


def list_of(table, narrow, lists, first, shape, axis):
    position = lax.broadcasted_iota(jnp.int32, shape, axis) + first
    found = jnp.zeros(shape, jnp.int32)
    for s in range(lists):
        found = found + (position >= table[narrow + s]).astype(jnp.int32)
    return found


def project(block, w_q, w_k, g):
    half = LANES // 2
    query = jnp.dot(block, w_q, preferred_element_type=f32) * half**-0.5
    key = jnp.dot(block, w_k, preferred_element_type=f32)
    turned = jnp.dot(block, g, preferred_element_type=f32).T
    return query.astype(bf16), key.astype(bf16), turned[:HEADS] + turned[half : half + HEADS]


def early_kernel(table, first, second, w_q, w_k, g, w_out, q_out, k_out, z_out):
    local = first.shape[0]
    own = w_q.shape[1]
    w_out[:, :own] = w_q[...]
    w_out[:, own:] = w_k[...]
    for m, block in enumerate((first, second)):
        rows = slice(m * local, (m + 1) * local)
        q_out[rows, :], k_out[rows, :], z_out[:, rows] = project(block[...], w_q[...], w_k[...], g[...])


def forward_kernel(table, *refs, narrow, lists):
    blocks, infos = refs[:narrow], refs[narrow : 2 * narrow]
    refs = refs[2 * narrow :]
    w, q_early, k_early, z_early, g, k_out, e_out, q_out, x_out, stat_out, part_out, z_out, lines_out = refs[:13]
    qs, kx, zt = refs[13:]
    local = blocks[0].shape[0]
    own = q_early.shape[1]
    heads = e_out.shape[0]
    half = LANES // 2
    step = pl.program_id(0)

    @pl.when(step == 0)
    def _():
        lane = lax.broadcasted_iota(jnp.int32, (local, LANES), 1)
        for m in range(narrow):
            rows = pl.ds(m * local, local)
            x_out[rows, :] = blocks[m][...]
            if m < 2:
                query, keys, turned = q_early[rows, :], k_early[rows, :], z_early[:, rows]
            else:
                query, keys, turned = project(blocks[m][...], w[:, :own], w[:, own:], g[...])
            qs[rows, :] = query
            k_out[rows, :] = keys
            zt[:, rows] = turned
            segment = list_of(table, narrow, lists, table[m] * local, (local, LANES), 0)
            away = jnp.where(lane == segment, 0.0, -far).astype(bf16)
            for p in range(heads // 2):
                kx[p, rows, :LANES] = keys[:, p * LANES : (p + 1) * LANES]
                kx[p, rows, LANES:] = away
            lines_out[:, rows] = infos[m][...]
            lines_out[2:3, rows] = list_of(table, narrow, lists, table[m] * local, (1, local), 1).astype(f32)
        z_out[...] = zt[...]

    at = pl.ds(pl.multiple_of(step * local, local), local)
    query = qs[at, :]
    q_out[...] = query
    lane = lax.broadcasted_iota(jnp.int32, (local, LANES), 1)
    segment = list_of(table, narrow, lists, table[step] * local, (local, LANES), 0)
    mine = (lane == segment).astype(f32).astype(bf16)
    stats = jnp.zeros((local, LANES), f32)
    zsum = jnp.zeros((local, 1), f32)
    for p in range(heads // 2):
        for s in range(2):
            h = 2 * p + s
            own = query[:, p * LANES : (p + 1) * LANES]
            own = jnp.where((lane >= half) == (s == 1), own, jnp.zeros_like(own))
            logits = contract(jnp.concatenate([own, mine], axis=1), kx[p], ((1,), (1,)))
            weights = jnp.exp2(logits * log2e)
            e_out[h] = weights.astype(bf16)
            zrow = zt[pl.ds(table[0] * heads + h, 1), :]
            inverse = 1.0 / jnp.sum(weights, axis=1, keepdims=True)
            zeta = jnp.sum(weights * zrow, axis=1, keepdims=True) * inverse
            stats = jnp.where(lane == h, zeta, stats)
            stats = jnp.where(lane == heads + h, inverse, stats)
            zsum = zsum + zeta
    stat_out[...] = stats
    part_out[...] = jnp.broadcast_to(zsum, (local, LANES)).T[:1]


def center_kernel(table, e, stat, key, z, a_out):
    heads = e.shape[0]
    rows = stat.shape[0]
    half = LANES // 2
    here = pl.ds(pl.multiple_of(pl.program_id(0) * rows, rows), rows)
    lane = lax.broadcasted_iota(jnp.int32, (rows, LANES), 1)
    stats = stat[...]
    for p in range(heads // 2):
        at = slice(p * LANES, (p + 1) * LANES)
        parts = []
        for h in (2 * p, 2 * p + 1):
            zrow = z[pl.ds(table[0] * heads + h, 1), :]
            centred = (e[h, here, :].astype(f32) * (zrow - stats[:, h : h + 1])).astype(bf16)
            part = jnp.dot(centred, key[:, at], preferred_element_type=f32)
            parts.append(part * stats[:, heads + h : heads + h + 1])
        a_out[:, at] = jnp.where(lane >= half, parts[1], parts[0]).astype(bf16)


def halves(blocks, pairs, wide_index, keep_out, send_out):
    odd = wide_index % 2 == 1
    for t in range(pairs):
        even, other = blocks(2 * t), blocks(2 * t + 1)
        place = jnp.bitwise_xor(t, wide_index // 2)
        keep_out[place] = jnp.where(odd, other, even).astype(bf16)
        send_out[place] = jnp.where(odd, even, other).astype(bf16)


def score_kernel(table, *refs, narrow, lists):
    partials = refs[:narrow]
    given, x, a, grad_out, keep_out, send_out, lines, acc = refs[narrow:]
    local, _ = a.shape
    scale = (LANES // 2) ** -0.5
    pairs, _, chunk = keep_out.shape
    step = pl.program_id(0)

    @pl.when(step == 0)
    def _():
        acc[...] = jnp.zeros_like(acc)
        lines[...] = given[...]
        for m in range(narrow):
            rows = pl.ds(m * local, local)
            summed = given[0:1, rows]
            for d in range(narrow):
                summed = summed + partials[d][:, (m ^ d) * local : ((m ^ d) + 1) * local]
            lines[0:1, rows] = summed

    at = pl.ds(pl.multiple_of(step * local, local), local)
    turned = jnp.concatenate([lines[:, at]] * (LANES // 8), axis=0).T
    same = turned[:, 2:3] == lines[2:3, :]
    gains = lines[1:2, :]
    spread = gains - turned[:, 1:2]
    margin = turned[:, 0:1] - lines[0:1, :]
    margin = jnp.where(spread > 0.0, margin, -margin)
    pulls = spread / (1.0 + jnp.exp(-margin))
    pulls = jnp.sum(jnp.where(same, pulls, 0.0), axis=1, keepdims=True)
    norm = jnp.sum(jnp.where(same, gains, 0.0), axis=1, keepdims=True)
    grad = loss_scale * pulls / norm
    grad_out[...] = grad
    query = (a[...].astype(f32) * (grad * scale)).astype(bf16)
    acc[...] += contract(query, x[at, :], ((0,), (0,)))

    @pl.when(step == pl.num_programs(0) - 1)
    def _():
        cut = lambda w: acc[:, w * chunk : (w + 1) * chunk]
        halves(cut, pairs, table[narrow + lists], keep_out, send_out)


def key_kernel(table, e, stat, query, z, grad, w_v, x, keys_out, keep_out, send_out, key_acc, c_acc, at_wide):
    heads, total, _ = e.shape
    rows = query.shape[0]
    half = LANES // 2
    own = query.shape[1]
    width = w_v.shape[0]
    pairs, lines, chunk = keep_out.shape
    step = pl.program_id(0)

    @pl.when(step == 0)
    def _():
        key_acc[...] = jnp.zeros_like(key_acc)
        c_acc[...] = jnp.zeros_like(c_acc)

    lane = lax.broadcasted_iota(jnp.int32, (rows, LANES), 1)
    stats = stat[...]
    here = pl.ds(pl.multiple_of(step * rows, rows), rows)
    for h in range(heads):
        p, s = h // 2, h % 2
        zeta = stats[:, h : h + 1]
        scaled = e[h, here, :].astype(f32) * (stats[:, heads + h : heads + h + 1] * grad[...])
        c_acc[h : h + 1, :] += jnp.sum(scaled, axis=0, keepdims=True)
        centred = (scaled * (z[pl.ds(table[0] * heads + h, 1), :] - zeta)).astype(bf16)
        head = query[:, p * LANES : (p + 1) * LANES]
        head = jnp.where((lane >= half) == (s == 1), head, jnp.zeros_like(head))
        key_acc[p * LANES : (p + 1) * LANES, :] += contract(head, centred, ((0,), (0,)))

    @pl.when(step == pl.num_programs(0) - 1)
    def _():
        c = c_acc[...]
        high = c.astype(bf16).astype(f32)
        parts = jnp.concatenate([high[:heads], (c - high)[:heads]], axis=0)
        extra = keys_out.shape[0] - own - 2 * heads
        parts = jnp.concatenate([parts, jnp.zeros((extra, total), f32)], axis=0)
        keys_out[:own] = key_acc[...].astype(bf16)
        keys_out[own:] = parts.astype(bf16)
        out = jnp.dot(keys_out[...], x[:, :width], preferred_element_type=f32)
        mass = out[own : own + heads] + out[own + heads : own + 2 * heads]
        high = mass.astype(bf16).astype(f32)
        tops = jnp.concatenate([high, mass - high], axis=0)
        values = jnp.dot(tops.astype(bf16), w_v[...], preferred_element_type=f32)
        values = values[:heads] + values[heads:]
        head = lax.broadcasted_iota(jnp.int32, (heads, own), 1) // half
        index = lax.broadcasted_iota(jnp.int32, (heads, own), 0)
        value = jnp.sum(jnp.where(head == index, values, 0.0), axis=0, keepdims=True)
        count = own // chunk
        cuts = [value[:, t * chunk : (t + 1) * chunk] for t in range(count)]
        fill = lines - own - heads - count
        cuts.append(jnp.zeros((fill, chunk), f32))

        def block(w):
            at = slice(w * chunk, (w + 1) * chunk)
            return jnp.concatenate([out[:own, at], mass[:, at]] + cuts, axis=0)

        halves(block, pairs, table[at_wide], keep_out, send_out)


def fetch(table, w, buffer, sems, first):
    narrow, _, own = buffer.shape
    copies = []
    for m in range(narrow):
        at = pl.ds(pl.multiple_of((table[m] + first) * own, own), own)
        copies.append(pltpu.make_async_copy(w.at[:, at], buffer.at[m], sems.at[m]))
        copies[m].start()
    return copies


def query_rows_kernel(table, *refs):
    *blocks, w, out, buffer, sems = refs
    copies = fetch(table, w, buffer, sems, 0)
    for m, block in enumerate(blocks):
        copies[m].wait()
        term = contract(block[...], buffer[m], ((1,), (1,)))
        out[...] = term if m == 0 else out[...] + term


def tail_kernel(table, *refs, narrow, heads):
    keys = refs[:narrow]
    w, query_rows, turned, source, incoming, grad, gain, score, out, acc, cs, buffer, sems = refs[narrow:]
    copies = fetch(table, w, buffer, sems, narrow)
    count, piece, width = out.shape
    own = width // narrow
    scale = (LANES // 2) ** -0.5
    acc[...] = query_rows[...] * (grad[...] * scale)
    for m in range(narrow):
        copies[m].wait()
        acc[...] += contract(keys[m][:own], buffer[m], ((0,), (1,)))
        mass = keys[m][own:].astype(f32)
        for h in range(heads):
            cs[pl.ds(table[m] * heads + h, 1), :] = mass[h : h + 1] + mass[heads + h : heads + h + 1]
    mass = cs[...]
    high = mass.astype(bf16).astype(f32)
    mass = jnp.concatenate([high, mass - high, high], axis=0).astype(bf16)
    acc[...] += contract(mass, turned[...], ((0,), (0,)))
    for c in range(count):
        part = pl.ds(c * piece, piece)
        scaled = acc[part, :] * gain[...]
        values = incoming[source[0, c], :, :width].astype(f32)
        inv = lax.rsqrt(jnp.mean(values * values, axis=1, keepdims=True) + epsilon)
        mean = jnp.mean(scaled * values, axis=1, keepdims=True)
        sums = grad[part, :] * score[...] + inv * scaled - values * (inv * inv * inv * mean)
        out[source[0, c]] = sums.astype(bf16)


def body(rows, grades, block_dest, block_source, lengths, gain, w_qkv, w_out, w_score):
    wide = lax.axis_size("wide")
    narrow = lax.axis_size("narrow")
    wide_index = lax.axis_index("wide")
    narrow_index = lax.axis_index("narrow")
    local, width = rows.shape
    lists = lengths.shape[1]
    piece = local // wide
    head_size = width // HEADS
    heads = HEADS // narrow
    own = heads * head_size
    total = local * narrow
    chunk = width // wide
    order = jnp.bitwise_xor(narrow_index, jnp.arange(narrow, dtype=jnp.int32))
    bounds = jnp.cumsum(lax.dynamic_index_in_dim(lengths, wide_index, 0, keepdims=False))
    table = jnp.concatenate([order, bounds.astype(jnp.int32), wide_index[None].astype(jnp.int32)])
    gain_row, score_row = gain[None, :], w_score[None, :]

    def swap(values, m):
        return lax.ppermute(values, "narrow", [(i, i ^ m) for i in range(narrow)])

    def across(values):
        return lax.all_to_all(values, "wide", split_axis=0, concat_axis=0, tiled=True)

    def spread(values):
        held = [values]
        for m in range(1, narrow):
            top = 1 << (m.bit_length() - 1)
            near_by = m ^ top
            held.append(swap(values, m) if near_by == 0 else None)
        for m in range(1, narrow):
            if held[m] is None:
                top = 1 << (m.bit_length() - 1)
                held[m] = swap(held[top], m ^ top)
        return held

    def shape(*dims, dtype=f32):
        return jax.ShapeDtypeStruct(dims, dtype)

    outgoing = call(
        pack_kernel, shape(wide, piece, width + LANES, dtype=bf16), [smem(), vmem(), vmem()]
    )(stay(block_dest), stay(rows.reshape(wide, piece, width)), stay(grades[None, :]))
    incoming = across(outgoing)

    u, g_turned, g_proj = call(
        prepare_kernel,
        (shape(width, 1), shape(3 * HEADS, width, dtype=bf16), shape(width, LANES, dtype=bf16)),
        [pl.BlockSpec((width, width), lambda i: (0, 2)), whole((width, width)), whole((1, width))],
        work=10**9,
        room=24,
        grid=(1,),
        out_specs=(whole((width, 1)), whole((3 * HEADS, width)), whole((width, LANES))),
    )(stay(w_qkv), w_out, score_row)

    normed, info = call(
        norm_kernel,
        (shape(wide, piece, width, dtype=bf16), shape(8, local)),
        [smem(), smem(), vmem(), vmem(), vmem(), pl.BlockSpec(memory_space=pl.ANY)],
        scratch_shapes=[pltpu.VMEM((local, LANES), f32)],
    )(block_source, table[None, :], near(incoming), gain_row, score_row, g_proj)
    blocks = spread(normed.reshape(local, width))
    infos = [info] + [swap(info, m) for m in range(1, narrow)]

    row_block = lambda columns: pl.BlockSpec((local, columns), lambda i, t: (i, 0))
    early = indexed(
        early_kernel,
        (
            shape(width, 2 * own, dtype=bf16),
            shape(2 * local, own, dtype=bf16),
            shape(2 * local, own, dtype=bf16),
            shape(HEADS, 2 * local),
        ),
        [
            vmem(),
            vmem(),
            pl.BlockSpec((width, own), lambda i, t: (0, t[0])),
            pl.BlockSpec((width, own), lambda i, t: (0, narrow + t[0])),
            vmem(),
        ],
        (vmem(),) * 4,
        (1,),
        work=10**9,
        room=10,
    )(table, near(blocks[0]), near(blocks[1]), stay(w_qkv), stay(w_qkv), near(g_proj))
    key, e, queries, x, stat, part, z, lines = indexed(
        lambda *refs: forward_kernel(*refs, narrow=narrow, lists=lists),
        (
            shape(total, own, dtype=bf16),
            shape(heads, total, total, dtype=bf16),
            shape(total, own, dtype=bf16),
            shape(total, width, dtype=bf16),
            shape(total, LANES),
            shape(1, total),
            shape(HEADS, total),
            shape(8, total),
        ),
        [vmem()] * (2 * narrow + 5),
        (
            whole((total, own)),
            pl.BlockSpec((heads, local, total), lambda i, t: (0, i, 0)),
            row_block(own),
            vmem(),
            row_block(LANES),
            pl.BlockSpec((1, local), lambda i, t: (0, i)),
            whole((HEADS, total)),
            whole((8, total)),
        ),
        (narrow,),
        [
            pltpu.VMEM((total, own), bf16),
            pltpu.VMEM((heads // 2, total, 2 * LANES), bf16),
            pltpu.VMEM((HEADS, total), f32),
        ],
        work=4 * 10**9,
        room=28,
    )(table, *map(near, [*blocks, *infos, *early, g_proj]))

    partials = [part] + [swap(part, m) for m in range(1, narrow)]
    a = indexed(
        center_kernel,
        shape(total, own, dtype=bf16),
        [vmem(), row_block(LANES), whole((total, own)), whole((HEADS, total))],
        row_block(own),
        (narrow,),
        work=2 * 10**9,
        room=10,
    )(table, near(e), stat, key, z)
    a_rows = [a[:local]] + [swap(a[m * local : (m + 1) * local], m) for m in range(1, narrow)]

    grad, keep_q, send_q = indexed(
        lambda *refs: score_kernel(*refs, narrow=narrow, lists=lists),
        (shape(total, 1),) + (shape(wide // 2, own, chunk, dtype=bf16),) * 2,
        [whole((1, total))] + [vmem()] * (narrow - 1) + [whole((8, total)), vmem(), row_block(own)],
        (row_block(1),) + (whole((wide // 2, own, chunk)),) * 2,
        (narrow,),
        [pltpu.VMEM((8, total), f32), pltpu.VMEM((own, width), f32)],
        work=2 * 10**9,
        room=14,
    )(table, partials[0], *map(near, partials[1:]), lines, near(x), a)

    def to_partner(values, step):
        return lax.ppermute(values, "wide", [(i, i ^ step) for i in range(wide)])

    def added(kept, received):
        return kept.astype(f32) + received.astype(f32)

    got_q = to_partner(send_q, 1)

    count_v = own // chunk
    lines_k = -(-(own + heads + count_v) // 16) * 16
    lines_c = -(-(own + 2 * heads) // 16) * 16
    keys, keep, send = indexed(
        lambda *refs: key_kernel(*refs, at_wide=narrow + lists),
        (shape(lines_c, total, dtype=bf16),) + (shape(wide // 2, lines_k, chunk, dtype=bf16),) * 2,
        [
            vmem(),
            row_block(LANES),
            row_block(own),
            whole((HEADS, total)),
            row_block(1),
            pl.BlockSpec((width, own), lambda i, t: (0, 2 * narrow + t[0])),
            vmem(),
        ],
        (whole((lines_c, total)),) + (whole((wide // 2, lines_k, chunk)),) * 2,
        (narrow,),
        [
            pltpu.VMEM((own, total), f32),
            pltpu.VMEM((8, total), f32),
        ],
        work=4 * 10**9,
        room=22,
    )(table, near(e), stat, queries, z, grad, stay(w_qkv), near(x))

    k_rows = [keys[:, :local]]
    k_rows += [swap(keys[:, m * local : (m + 1) * local], m) for m in range(1, narrow)]
    got_k = to_partner(send, 1)
    sums = jnp.concatenate([added(keep_q, got_q), added(keep, got_k)], axis=1)
    step = 2
    while step < wide:
        cut = sums.astype(bf16).reshape(-1, 2, own + lines_k, chunk)
        sums = added(cut[:, 0], to_partner(cut[:, 1], step))
        step *= 2
    sums = sums[0].astype(bf16)

    fetched = [pltpu.VMEM((narrow, width, own), bf16), pltpu.SemaphoreType.DMA((narrow,))]
    anywhere = pl.BlockSpec(memory_space=pl.ANY)
    query_rows = indexed(
        query_rows_kernel,
        shape(local, width),
        [vmem()] * narrow + [anywhere],
        vmem(),
        (),
        fetched,
        work=10**9,
    )(table, *map(near, a_rows), stay(w_qkv))
    returning = indexed(
        lambda *refs: tail_kernel(*refs, narrow=narrow, heads=heads),
        shape(wide, piece, width, dtype=bf16),
        [vmem()] * narrow + [anywhere] + [vmem()] * 2 + [smem()] + [vmem()] * 4,
        vmem(),
        (),
        [pltpu.VMEM((local, width), f32), pltpu.VMEM((HEADS, local), f32)] + fetched,
        work=10**9,
        room=10,
    )(
        table, *map(near, k_rows), stay(w_qkv), near(query_rows), g_turned, block_source,
        near(incoming), grad[:local], gain_row, score_row,
    )
    arrived = across(returning)
    grad_rows = arrived[block_dest[0]].reshape(local, width)

    gathered = jnp.stack(spread(sums))[order]
    q_cols = gathered[:, :own].reshape(width, chunk)
    gathered = gathered[:, own:]
    k_cols = gathered[:, :own].reshape(width, chunk)
    m_all = gathered[:, own : own + heads].astype(f32)
    m_rows = jnp.broadcast_to(m_all.reshape(HEADS, 1, chunk), (HEADS, head_size, chunk))
    v_cols = (m_rows.reshape(width, chunk) * u).astype(bf16)
    v_all = gathered[:, own + heads : own + heads + count_v].astype(f32)
    v_all = v_all.reshape(width)
    columns = 3 * width // (wide * narrow)
    full = jnp.concatenate([q_cols, k_cols, v_cols], axis=0).reshape(wide, narrow, columns, chunk)
    mine = lax.dynamic_index_in_dim(full, narrow_index, 1, keepdims=False)
    parts = across(mine)
    grad_qkv = parts.astype(f32).transpose(0, 2, 1).reshape(width, columns)
    out_columns = width // (wide * narrow)
    place = (wide_index * narrow + narrow_index) * out_columns
    grad_out = v_all[:, None] * lax.dynamic_slice_in_dim(w_score, place, out_columns)[None, :]
    return (grad_rows, grad_qkv, grad_out)


def solution(mesh):
    both = ("wide", "narrow")
    placed = (P(both, None), P(both), P(both, None), P(both, None), P(), P(), P(), P(), P())
    return jax.shard_map(
        body,
        mesh=mesh,
        in_specs=placed,
        out_specs=(P(both, None), P(None, both), P(None, both)),
        check_vma=False,
    )
```
